256 devices in a mesh: gx: 16 (over y, z_hi), gy: 8 (over x, core), gz: 2 (over z_lo).
Axes of the slice: x: 4, y: 4, z: 8 (z_hi: 4, z_lo: 2; z = z_hi * 2 + z_lo), core: 2. Of those that a mesh axis runs over, the one named last changes fastest.
Arguments:
- fraction: float32 [64, 1024, 1024], P('gx', 'gy', 'gz'), may hold values from 0 to 1
- orientation: int32 [64, 1024, 1024], P('gx', 'gy', 'gz'), may hold values from 0 to 2
- interface: int32 [64, 1024, 1024], P('gx', 'gy', 'gz'), may hold values from 0 to 1
Outputs:
- curvature: float32 [64, 1024, 1024], P('gx', 'gy', 'gz')
- peak: float32 [], replicated
The draws below stay inside these ranges and needn't reach their ends.
All inputs are finite; a program needn't handle non-finite values.
Results may differ from the reference program's by a relative error of at most 0.0003.
Values sent between devices are 32-bit elements; how exact they have to be, the bound alone decides.
A program may use at most 64 MiB of HBM per device.

```python
import jax
import jax.numpy as jnp
from jax import lax

NX = 64
NY = 1024
NZ = 1024


def draw_interface(key, part):
    shape = (NX, NY, NZ)
    planes = lax.broadcasted_iota(jnp.int32, shape, 0)
    threshold = 50 + 550 * planes // NX
    rolled = jax.random.randint(key, shape, 0, 1000, dtype=jnp.int32)
    return (rolled < threshold).astype(jnp.int32)


def plant(entries, stream_key, smallest, largest):
    index_at = [jax.random.randint(jax.random.fold_in(stream_key, axis), (), 0, length) for axis, length in enumerate(entries.shape)]
    longest = entries.shape.index(max(entries.shape))
    beside = index_at[:longest] + [(index_at[longest] + 1) % entries.shape[longest]] + index_at[longest + 1:]
    return entries.at[tuple(index_at)].set(smallest).at[tuple(beside)].set(largest)


def levels(key, dims, pieces, smallest, top_value):
    gain = 1.0
    for position, shards_of in pieces:
        steps = jax.random.uniform(jax.random.fold_in(jax.random.fold_in(key, 6), position), (shards_of,), jnp.float32, smallest / len(pieces), top_value / len(pieces))
        gain = gain * jnp.repeat(jnp.exp(steps), dims[position] // shards_of).reshape((-1,) + (1,) * (len(dims) - 1 - position))
    return gain


def setup_inputs(seed: int = 0) -> dict:
    arg_keys = jax.random.split(jax.random.key(seed), 4)
    return {
        "fraction": jnp.clip(1.0 * jax.random.uniform(arg_keys[0], (NX, NY, NZ), jnp.float32) ** levels(arg_keys[0], (NX, NY, NZ), ((0, 16), (1, 8), (2, 2)), -0.2, 0.2), 0.0, 1.0),
        "orientation": plant(jax.random.randint(arg_keys[1], (NX, NY, NZ), 0, 3), jax.random.fold_in(arg_keys[1], 1), 0, 2).astype(jnp.int32),
        "interface": draw_interface(jax.random.fold_in(arg_keys[3], 71), 0),
    }


def curvature_block(padded, orientation, interface):
    shape = orientation.shape
    results = []
    for axis in range(3):
        others = [other for other in range(3) if other != axis]
        column = lax.slice_in_dim(padded, 0, shape[axis], axis=axis)
        for step in range(1, 7):
            column = column + lax.slice_in_dim(padded, step, step + shape[axis], axis=axis)

        def height(first, second):
            starts = [3, 3, 3]
            starts[axis] = 0
            starts[others[0]] += first
            starts[others[1]] += second
            return lax.slice(column, starts, [st + sz for st, sz in zip(starts, shape)])
        centre = height(0, 0)
        plus_a, minus_a = (height(1, 0), height(-1, 0))
        plus_b, minus_b = (height(0, 1), height(0, -1))
        slope_a = 0.5 * (plus_a - minus_a)
        slope_b = 0.5 * (plus_b - minus_b)
        bend_a = plus_a - 2.0 * centre + minus_a
        bend_b = plus_b - 2.0 * centre + minus_b
        twist = 0.25 * (height(1, 1) - height(1, -1) - height(-1, 1) + height(-1, -1))
        numer = bend_a * (1.0 + slope_b * slope_b) + bend_b * (1.0 + slope_a * slope_a) - 2.0 * twist * slope_a * slope_b
        denom = 1.0 + slope_a * slope_a + slope_b * slope_b
        results.append(numer / (denom * jnp.sqrt(denom)))
    picked = jnp.where(orientation == 0, results[0], jnp.where(orientation == 1, results[1], results[2]))
    return jnp.where(interface == 1, picked, jnp.zeros_like(picked))

def reference(fraction, orientation, interface):
    padded = jnp.pad(fraction, 3)
    slab = 8
    count = NX // slab
    orient_slabs = orientation.reshape(count, slab, NY, NZ)
    flag_slabs = interface.reshape(count, slab, NY, NZ)

    def one_slab(index):
        start = (index * slab).astype(jnp.int32)
        piece = lax.dynamic_slice_in_dim(padded, start, slab + 6, 0)
        return curvature_block(piece, orient_slabs[index], flag_slabs[index])
    blocks = lax.map(one_slab, jnp.arange(count, dtype=jnp.int32))
    curvature = blocks.reshape(NX, NY, NZ)
    return (curvature, jnp.max(jnp.abs(curvature)))
```

```python
import functools

import jax
import jax.numpy as jnp
from jax import lax
from jax.experimental import pallas as pl
from jax.experimental.pallas import tpu as pltpu
from jax.sharding import PartitionSpec as P

MESH = pl.DeviceIdType.MESH
LANES = 128
Z_HI = 4


def shifted(tiles, rolled, shift, lane):
    count = len(rolled)
    out = []
    for t in range(tiles):
        if shift > 0:
            out.append(jnp.where(lane >= LANES - shift, rolled[(t + 1) % count], rolled[t]))
        else:
            out.append(jnp.where(lane < -shift, rolled[(t - 1) % count], rolled[t]))
    return out


def roll_all(tiles, shift):
    return [pltpu.roll(x, (-shift) % LANES, x.ndim - 1) for x in tiles]


def kernel(
    sizes, f_hbm, ori_hbm, itf_hbm, out_hbm, peak_ref,
    ext, c0, d0, s0, c2, ori, itf, res, zs, zr, vmax, r1, r2,
    load_sem, store_sem, xs, xr, ys, yr, y4s, y4r, yxs, yxr, zss, zrs, r1s, r1r, r2s, r2r,
):
    ngx, ngy, ngz, zhi = sizes
    gx, gy, gz = lax.axis_index("gx"), lax.axis_index("gy"), lax.axis_index("gz")
    other = 1 - gz
    planes, rows, lanes = f_hbm.shape
    nt = lanes // LANES
    nr = rows // 8
    has_lo, has_hi = gx > 0, gx < ngx - 1
    y_lo, y_hi = gy > 0, gy < ngy - 1
    top = 8 + rows

    loads = [
        pltpu.make_async_copy(
            f_hbm.at[:, :, pl.ds(t * LANES, LANES)], ext.at[pl.ds(3, 4), t, pl.ds(8, rows), :],
            load_sem.at[t])
        for t in range(nt)
    ]
    load_ori = pltpu.make_async_copy(ori_hbm, ori, load_sem.at[nt])
    load_itf = pltpu.make_async_copy(itf_hbm, itf, load_sem.at[nt + 1])
    for copy in loads:
        copy.start()
    load_ori.start()
    load_itf.start()

    @pl.when(jnp.logical_not(has_lo))
    def _():
        ext[0:3] = jnp.zeros((3, nt + 1, rows + 16, LANES), jnp.float32)

    @pl.when(jnp.logical_not(has_hi))
    def _():
        ext[7:10] = jnp.zeros((3, nt + 1, rows + 16, LANES), jnp.float32)

    @pl.when(jnp.logical_not(y_lo))
    def _():
        ext[:, :, 0:8] = jnp.zeros((10, nt + 1, 8, LANES), jnp.float32)

    @pl.when(jnp.logical_not(y_hi))
    def _():
        ext[:, :, top:top + 8] = jnp.zeros((10, nt + 1, 8, LANES), jnp.float32)

    ny = ngx // zhi
    y_at, z_at = gx // zhi, gx % zhi
    n1, n2 = zhi * ngz, ny * ngy
    me1 = z_at * ngz + gz
    me2 = y_at * ngy + gy

    def peer1(d):
        i = lax.rem(me1 + d, n1)
        return (y_at * zhi + i // ngz, gy, lax.rem(i, ngz))

    def peer2(d):
        i = lax.rem(me2 + d, n2)
        return ((i // ngy) * zhi + z_at, lax.rem(i, ngy), gz)

    barrier = pltpu.get_barrier_semaphore()

    def greet(device):
        pl.semaphore_signal(barrier, inc=1, device_id=device, device_id_type=MESH)

    cross_hi = jnp.logical_and(has_hi, z_at == zhi - 1)
    cross_lo = jnp.logical_and(has_lo, z_at == 0)

    @pl.when(cross_hi)
    def _():
        greet((gx + 1, gy, gz))
        greet((gx + 1, gy, other))

    @pl.when(cross_lo)
    def _():
        greet((gx - 1, gy, gz))
        greet((gx - 1, gy, other))

    for d in range(1, n1):
        greet(peer1(d))
    for d in range(1, n2):
        greet(peer2(d))

    for copy in loads:
        copy.wait()

    edge = jnp.where(gz == 0, nt - 1, 0)
    for p in range(4):
        turned = jnp.transpose(ext[3 + p, edge, 8:top, :])
        zs[p] = jnp.where(gz == 0, turned[LANES - 8:LANES], turned[0:8])
    vmax[...] = jnp.zeros_like(vmax)

    greeted = n1 - 1 + n2 - 1 + jnp.where(cross_hi, 2, 0) + jnp.where(cross_lo, 2, 0)
    pl.semaphore_wait(barrier, greeted)

    def remote(src, dst, send, recv, device):
        return pltpu.make_async_remote_copy(
            src_ref=src, dst_ref=dst, send_sem=send, recv_sem=recv, device_id=device,
            device_id_type=MESH)

    z_own = remote(zs, zr.at[pl.ds(3, 4)], zss.at[0], zrs.at[0], (gx, gy, other))
    z_up = remote(zs.at[pl.ds(1, 3)], zr.at[pl.ds(0, 3)], zss.at[1], zrs.at[1], (gx + 1, gy, other))
    z_dn = remote(zs.at[pl.ds(0, 3)], zr.at[pl.ds(7, 3)], zss.at[2], zrs.at[2], (gx - 1, gy, other))

    def x_up(r):
        at = pl.ds(pl.multiple_of(8 + r * 8, 8), 8)
        return remote(ext.at[pl.ds(4, 3), pl.ds(0, nt), at, :], ext.at[pl.ds(0, 3), pl.ds(0, nt), at, :],
                      xs.at[0, r], xr.at[0, r], (gx + 1, gy, gz))

    def x_dn(r):
        at = pl.ds(pl.multiple_of(8 + r * 8, 8), 8)
        return remote(ext.at[pl.ds(3, 3), pl.ds(0, nt), at, :], ext.at[pl.ds(7, 3), pl.ds(0, nt), at, :],
                      xs.at[1, r], xr.at[1, r], (gx - 1, gy, gz))

    def y_up(first, count, t0, tn, send, recv):
        return remote(ext.at[pl.ds(first, count), pl.ds(t0, tn), pl.ds(rows, 8), :],
                      ext.at[pl.ds(first, count), pl.ds(t0, tn), pl.ds(0, 8), :], send, recv,
                      (gx, gy + 1, gz))

    def y_dn(first, count, t0, tn, send, recv):
        return remote(ext.at[pl.ds(first, count), pl.ds(t0, tn), pl.ds(8, 8), :],
                      ext.at[pl.ds(first, count), pl.ds(t0, tn), pl.ds(top, 8), :], send, recv,
                      (gx, gy - 1, gz))

    y_own = (y_up(3, 4, 0, nt, ys.at[0], yr.at[0]), y_dn(3, 4, 0, nt, ys.at[1], yr.at[1]))
    y_edge = (y_up(0, 10, nt, 1, y4s.at[0], y4r.at[0]), y_dn(0, 10, nt, 1, y4s.at[1], y4r.at[1]))
    y_far = [
        (y_up(first, 3, 0, nt, yxs.at[0, s], yxr.at[0, s]), y_dn(first, 3, 0, nt, yxs.at[1, s], yxr.at[1, s]))
        for s, first in ((0, 0), (1, 7))
    ]

    z_own.start()

    @pl.when(has_hi)
    def _():
        z_up.start()
        x_up(0).start()
        x_up(nr - 1).start()

    @pl.when(has_lo)
    def _():
        z_dn.start()
        x_dn(0).start()
        x_dn(nr - 1).start()

    @pl.when(y_hi)
    def _():
        y_own[0].start()

    @pl.when(y_lo)
    def _():
        y_own[1].start()

    def send_row(r, carry):
        @pl.when(has_hi)
        def _():
            x_up(r).start()

        @pl.when(has_lo)
        def _():
            x_dn(r).start()

        return carry

    lax.fori_loop(1, nr - 1, send_row, 0)

    def take_z(first, count):
        for p in range(first, first + count):
            part = zr[p]
            zero = jnp.zeros_like(part)
            low, high = jnp.where(gz == 0, part, zero), jnp.where(gz == 0, zero, part)
            middle = jnp.zeros((LANES - 16, LANES), jnp.float32)
            ext[p, nt, 8:top, :] = jnp.transpose(jnp.concatenate([low, middle, high], axis=0))

    z_own.wait_recv()
    take_z(3, 4)

    @pl.when(has_lo)
    def _():
        z_up.wait_recv()
        take_z(0, 3)

    @pl.when(has_hi)
    def _():
        z_dn.wait_recv()
        take_z(7, 3)

    def arrived(r):
        @pl.when(has_lo)
        def _():
            x_up(r).wait_recv()

        @pl.when(has_hi)
        def _():
            x_dn(r).wait_recv()

    arrived(0)
    arrived(nr - 1)

    for ok, k in ((y_hi, 0), (y_lo, 1)):
        @pl.when(ok)
        def _(k=k):
            y_edge[k].start()

        @pl.when(jnp.logical_and(ok, has_lo))
        def _(k=k):
            y_far[0][k].start()

        @pl.when(jnp.logical_and(ok, has_hi))
        def _(k=k):
            y_far[1][k].start()

    lane = lax.broadcasted_iota(jnp.int32, (8, LANES), 1)

    def columns(tile):
        at = pl.ds(pl.multiple_of(tile * 8, 8), 8)
        sums = []
        for t in range(nt + 1):
            e = [ext[p, t, at, :] for p in range(10)]
            mid = (e[3] + e[4]) + (e[5] + e[6])
            lo2, hi2 = e[2] + e[1], e[7] + e[8]
            sums.append([mid + (lo2 + e[0]), mid + lo2 + e[7], mid + e[2] + hi2, mid + (hi2 + e[9])])
        for x in range(4):
            h = [sums[t][x] for t in range(nt + 1)]
            after = shifted(nt, roll_all(h, 1), 1, lane)
            before = shifted(nt, roll_all(h, -1), -1, lane)
            for t in range(nt):
                c0[x, t, at, :] = h[t]
                d0[x, t, at, :] = after[t] - before[t]
                s0[x, t, at, :] = after[t] + before[t] - 2.0 * h[t]
        for p in range(6):
            f = [ext[2 + p, t, at, :] for t in range(nt + 1)]
            pair = [a + b for a, b in zip(f, shifted(nt + 1, roll_all(f, 1), 1, lane))]
            quad = [a + b for a, b in zip(pair, shifted(nt + 1, roll_all(pair, 2), 2, lane))]
            back = shifted(nt, roll_all(quad, -3), -3, lane)
            for t in range(nt):
                c2[p, t, at, :] = back[t] + (quad[t] - f[t])

    def curve(tile):
        row = tile * 8
        own = pl.ds(pl.multiple_of(row - 8, 8), 8)
        at = pl.ds(pl.multiple_of(row, 8), 8)
        up, dn = pl.ds(row + 1, 8), pl.ds(row - 1, 8)
        col = []
        for p in range(6):
            parts = []
            for t in range(nt + 1):
                v = [ext[2 + p, t, pl.ds(row + k, 8), :] for k in range(-3, 4)]
                parts.append(((v[0] + v[1]) + (v[2] + v[3])) + ((v[4] + v[5]) + v[6]))
            after = shifted(nt, roll_all(parts, 1), 1, lane)
            before = shifted(nt, roll_all(parts, -1), -1, lane)
            col.append((parts, [a - b for a, b in zip(after, before)], [a + b for a, b in zip(after, before)]))
        best = vmax[...]
        for t in range(nt):
            across = pl.ds(t * LANES, LANES)
            for x in range(4):
                o = ori[x, own, across]
                is0, is1 = o == 0, o == 1

                def pick(a, b, c):
                    return jnp.where(is0, a, jnp.where(is1, b, c))

                h0 = c0[x, t, at, :]
                u0, w0 = c0[x, t, up, :], c0[x, t, dn, :]
                h1 = col[x + 1][0][t]
                u1, w1 = col[x + 2][0][t], col[x][0][t]
                h2 = c2[x + 1, t, at, :]
                u2, w2 = c2[x + 2, t, at, :], c2[x, t, at, :]
                b2u, b2w = c2[x + 1, t, up, :], c2[x + 1, t, dn, :]
                twist2 = (c2[x + 2, t, up, :] - c2[x + 2, t, dn, :]) - (c2[x, t, up, :] - c2[x, t, dn, :])
                centre = pick(h0, h1, h2)
                plus, minus = pick(u0, u1, u2), pick(w0, w1, w2)
                slope_a = 0.5 * (plus - minus)
                bend_a = plus + minus - 2.0 * centre
                slope_b = 0.5 * pick(d0[x, t, at, :], col[x + 1][1][t], b2u - b2w)
                bend_b = pick(s0[x, t, at, :], col[x + 1][2][t] - 2.0 * h1, b2u + b2w - 2.0 * h2)
                twist = pick(d0[x, t, up, :] - d0[x, t, dn, :], col[x + 2][1][t] - col[x][1][t], twist2)
                qa, qb = slope_a * slope_a, slope_b * slope_b
                numer = bend_a * (1.0 + qb) + bend_b * (1.0 + qa) - 0.5 * twist * (slope_a * slope_b)
                inv = lax.rsqrt(1.0 + qa + qb)
                kappa = jnp.where(itf[x, own, across] == 1, numer * (inv * inv * inv), 0.0)
                res[x, own, across] = kappa
                best = jnp.maximum(best, jnp.abs(kappa))
        vmax[...] = best

    def store(tile):
        own = pl.ds(pl.multiple_of(tile * 8 - 8, 8), 8)
        return pltpu.make_async_copy(res.at[:, own, :], out_hbm.at[:, own, :], store_sem.at[tile - 1])

    for ok, k in ((y_lo, 0), (y_hi, 1)):
        @pl.when(ok)
        def _(k=k):
            y_own[k].wait_recv()
            y_edge[k].wait_recv()

        @pl.when(jnp.logical_and(ok, has_lo))
        def _(k=k):
            y_far[0][k].wait_recv()

        @pl.when(jnp.logical_and(ok, has_hi))
        def _(k=k):
            y_far[1][k].wait_recv()

    load_ori.wait()
    load_itf.wait()

    def edges(i, carry):
        columns(i + jnp.where(i >= 2, nr - 2, 0))
        return carry

    lax.fori_loop(0, 4, edges, 0)

    def middle(tile, carry):
        arrived(tile - 1)
        columns(tile)
        curve(tile - 1)
        store(tile - 1).start()
        return carry

    lax.fori_loop(2, nr, middle, 0)

    def tail(tile, carry):
        curve(tile)
        store(tile).start()
        return carry

    lax.fori_loop(nr - 1, nr + 1, tail, 0)

    r1[me1] = jnp.max(vmax[...], axis=0, keepdims=True)

    def red1(d):
        return remote(r1.at[me1], r1.at[me1], r1s.at[d], r1r.at[d], peer1(d))

    def red2(d):
        return remote(r2.at[me2], r2.at[me2], r2s.at[d], r2r.at[d], peer2(d))

    def recv1(d):
        return remote(r1.at[lax.rem(me1 - d + n1, n1)], r1.at[lax.rem(me1 - d + n1, n1)], r1s.at[d], r1r.at[d], peer1(d))

    def recv2(d):
        return remote(r2.at[lax.rem(me2 - d + n2, n2)], r2.at[lax.rem(me2 - d + n2, n2)], r2s.at[d], r2r.at[d], peer2(d))

    for d in range(1, n1):
        red1(d).start()
    for d in range(1, n1):
        recv1(d).wait_recv()
    r2[me2] = jnp.max(r1[...], axis=0)
    for d in range(1, n2):
        red2(d).start()

    z_own.wait_send()

    def sent_row(r, carry):
        @pl.when(has_hi)
        def _():
            x_up(r).wait_send()

        @pl.when(has_lo)
        def _():
            x_dn(r).wait_send()

        store(r + 1).wait()
        return carry

    lax.fori_loop(0, nr, sent_row, 0)

    @pl.when(has_hi)
    def _():
        z_up.wait_send()

    @pl.when(has_lo)
    def _():
        z_dn.wait_send()

    for ok, k in ((y_hi, 0), (y_lo, 1)):
        @pl.when(ok)
        def _(k=k):
            y_own[k].wait_send()
            y_edge[k].wait_send()

        @pl.when(jnp.logical_and(ok, has_lo))
        def _(k=k):
            y_far[0][k].wait_send()

        @pl.when(jnp.logical_and(ok, has_hi))
        def _(k=k):
            y_far[1][k].wait_send()

    for d in range(1, n1):
        red1(d).wait_send()
    for d in range(1, n2):
        recv2(d).wait_recv()
    peak_ref[0, 0] = jnp.max(r2[...])
    for d in range(1, n2):
        red2(d).wait_send()


def block(sizes, fraction, orientation, interface):
    planes, rows, lanes = fraction.shape
    ngx, ngy, ngz, zhi = sizes
    nt, nr = lanes // LANES, rows // 8
    n1, n2 = zhi * ngz, (ngx // zhi) * ngy
    dma = pltpu.SemaphoreType.DMA
    f32 = jnp.float32
    curvature, peak = pl.pallas_call(
        functools.partial(kernel, sizes),
        out_shape=(
            jax.ShapeDtypeStruct(fraction.shape, f32),
            jax.ShapeDtypeStruct((1, 1), f32),
        ),
        in_specs=[pl.BlockSpec(memory_space=pl.ANY)] * 3,
        out_specs=(pl.BlockSpec(memory_space=pl.ANY), pl.BlockSpec(memory_space=pltpu.SMEM)),
        scratch_shapes=[
            pltpu.VMEM((10, nt + 1, rows + 16, LANES), f32),
            pltpu.VMEM((4, nt, rows + 16, LANES), f32),
            pltpu.VMEM((4, nt, rows + 16, LANES), f32),
            pltpu.VMEM((4, nt, rows + 16, LANES), f32),
            pltpu.VMEM((6, nt, rows + 16, LANES), f32),
            pltpu.VMEM((planes, rows, lanes), jnp.int32),
            pltpu.VMEM((planes, rows, lanes), jnp.int32),
            pltpu.VMEM((planes, rows, lanes), f32),
            pltpu.VMEM((4, 8, LANES), f32),
            pltpu.VMEM((10, 8, LANES), f32),
            pltpu.VMEM((8, LANES), f32),
            pltpu.VMEM((n1, 1, LANES), f32),
            pltpu.VMEM((n2, 1, LANES), f32),
            dma((nt + 2,)), dma((nr,)),
            dma((2, nr)), dma((2, nr)),
            dma((2,)), dma((2,)),
            dma((2,)), dma((2,)),
            dma((2, 2)), dma((2, 2)),
            dma((3,)), dma((3,)),
            dma((n1,)), dma((n1,)),
            dma((n2,)), dma((n2,)),
        ],
        compiler_params=pltpu.CompilerParams(
            collective_id=0, has_side_effects=True, vmem_limit_bytes=62 * 1024 * 1024
        ),
    )(fraction, orientation, interface)
    return curvature, peak.reshape(())


def solution(mesh):
    sizes = (mesh.shape["gx"], mesh.shape["gy"], mesh.shape["gz"], min(Z_HI, mesh.shape["gx"]))
    spec = P("gx", "gy", "gz")
    return jax.shard_map(
        functools.partial(block, sizes), mesh=mesh, in_specs=(spec,) * 3, out_specs=(spec, P()), check_vma=False
    )
```

```python
import functools

import jax
import jax.numpy as jnp
from jax import lax
from jax.experimental import pallas as pl
from jax.experimental.pallas import tpu as pltpu
from jax.sharding import PartitionSpec as P

MESH = pl.DeviceIdType.MESH
LANES = 128
Z_HI = 4


def shifted(tiles, rolled, shift, lane):
    count = len(rolled)
    out = []
    for t in range(tiles):
        if shift > 0:
            out.append(jnp.where(lane >= LANES - shift, rolled[(t + 1) % count], rolled[t]))
        else:
            out.append(jnp.where(lane < -shift, rolled[(t - 1) % count], rolled[t]))
    return out


def roll_all(tiles, shift):
    return [pltpu.roll(x, (-shift) % LANES, x.ndim - 1) for x in tiles]


def kernel(
    sizes, f_hbm, ori_hbm, itf_hbm, res, peak_ref,
    ext, c0, d0, s0, c2, ori, itf, zs, zr, zt, vmax, r1, r2,
    load_sem, xs, xr, ys, yr, y4s, y4r, yxs, yxr, zss, zrs, r1s, r1r, r2s, r2r, tok,
):
    ngx, ngy, ngz, zhi = sizes
    gx, gy, gz = lax.axis_index("gx"), lax.axis_index("gy"), lax.axis_index("gz")
    other = 1 - gz
    planes, rows, lanes = f_hbm.shape
    nt = lanes // LANES
    nr = rows // 8
    has_lo, has_hi = gx > 0, gx < ngx - 1
    y_lo, y_hi = gy > 0, gy < ngy - 1
    top = 8 + rows

    loads = [
        pltpu.make_async_copy(
            f_hbm.at[:, :, pl.ds(t * LANES, LANES)], ext.at[pl.ds(3, 4), t, pl.ds(8, rows), :],
            load_sem.at[t])
        for t in range(nt)
    ]
    load_ori = pltpu.make_async_copy(ori_hbm, ori, load_sem.at[nt])
    load_itf = pltpu.make_async_copy(itf_hbm, itf, load_sem.at[nt + 1])
    for copy in loads:
        copy.start()
    load_ori.start()
    load_itf.start()

    ny = ngx // zhi
    y_at, z_at = gx // zhi, gx % zhi
    n1, n2 = zhi * ngz, ny * ngy
    me1 = z_at * ngz + gz
    me2 = y_at * ngy + gy

    def peer1(d):
        i = lax.rem(me1 + d, n1)
        return (y_at * zhi + i // ngz, gy, lax.rem(i, ngz))

    def peer2(d):
        i = lax.rem(me2 + d, n2)
        return ((i // ngy) * zhi + z_at, lax.rem(i, ngy), gz)

    nx, x_at, core = ngy // 2, gy // 2, lax.rem(gy, 2)

    def steps(n):
        return (1, n - 1) if n > 2 else (1,) * (n - 1)

    ring = [(y_at * zhi + lax.rem(z_at + d, zhi), gy, gz) for d in steps(zhi)]
    ring += [(lax.rem(y_at + d, ny) * zhi + z_at, gy, gz) for d in steps(ny)]
    ring += [(gx, lax.rem(x_at + d, nx) * 2 + core, gz) for d in steps(nx)]
    ring += [(gx, gy, other), (gx, gy + 1 - 2 * core, gz)]
    barrier = pltpu.get_barrier_semaphore()

    def tell(semaphore, device):
        pl.semaphore_signal(semaphore, inc=1, device_id=device, device_id_type=MESH)

    extra = (
        (jnp.logical_and(has_hi, z_at == zhi - 1), (gx + 1, gy, gz)),
        (jnp.logical_and(has_lo, z_at == 0), (gx - 1, gy, gz)),
        (jnp.logical_and(y_hi, core == 1), (gx, gy + 1, gz)),
        (jnp.logical_and(y_lo, core == 0), (gx, gy - 1, gz)),
    )
    for ok, device in extra:
        @pl.when(ok)
        def _(device=device):
            tell(barrier, device)

    for device in ring:
        tell(barrier, device)
    greeted = len(ring)
    for ok, _ in extra:
        greeted = greeted + jnp.where(ok, 1, 0)

    @pl.when(jnp.logical_not(has_lo))
    def _():
        ext[0:3] = jnp.zeros((3, nt + 1, rows + 16, LANES), jnp.float32)

    @pl.when(jnp.logical_not(has_hi))
    def _():
        ext[7:10] = jnp.zeros((3, nt + 1, rows + 16, LANES), jnp.float32)

    @pl.when(jnp.logical_not(y_lo))
    def _():
        ext[:, :, 0:8] = jnp.zeros((10, nt + 1, 8, LANES), jnp.float32)

    @pl.when(jnp.logical_not(y_hi))
    def _():
        ext[:, :, top:top + 8] = jnp.zeros((10, nt + 1, 8, LANES), jnp.float32)

    for copy in loads:
        copy.wait()

    edge = jnp.where(gz == 0, nt - 1, 0)
    for p in range(4):
        turned = jnp.transpose(ext[3 + p, edge, 8:top, :])
        part = jnp.where(gz == 0, turned[LANES - 3:LANES], turned[0:3])
        for c in range(3):
            zs[p, c] = part[c:c + 1]
    zt[...] = jnp.zeros_like(zt)
    vmax[...] = jnp.zeros_like(vmax)

    pl.semaphore_wait(barrier, greeted)

    def remote(src, dst, send, recv, device):
        return pltpu.make_async_remote_copy(
            src_ref=src, dst_ref=dst, send_sem=send, recv_sem=recv, device_id=device,
            device_id_type=MESH)

    nearest = 2 * gz
    z_own = remote(zs, zr.at[pl.ds(3, 4)], zss.at[0], zrs.at[0], (gx, gy, other))
    z_up = (
        remote(zr.at[6], zr.at[2], zss.at[1], zrs.at[1], (gx + 1, gy, gz)),
        remote(zr.at[pl.ds(4, 2), nearest], zr.at[pl.ds(0, 2), nearest], zss.at[2], zrs.at[2], (gx + 1, gy, gz)),
    )
    z_dn = (
        remote(zr.at[3], zr.at[7], zss.at[3], zrs.at[3], (gx - 1, gy, gz)),
        remote(zr.at[pl.ds(4, 2), nearest], zr.at[pl.ds(8, 2), nearest], zss.at[4], zrs.at[4], (gx - 1, gy, gz)),
    )

    def x_up(r):
        at = pl.ds(pl.multiple_of(8 + r * 8, 8), 8)
        return remote(ext.at[pl.ds(4, 3), pl.ds(0, nt), at, :], ext.at[pl.ds(0, 3), pl.ds(0, nt), at, :],
                      xs.at[0, r], xr.at[0, r], (gx + 1, gy, gz))

    def x_dn(r):
        at = pl.ds(pl.multiple_of(8 + r * 8, 8), 8)
        return remote(ext.at[pl.ds(3, 3), pl.ds(0, nt), at, :], ext.at[pl.ds(7, 3), pl.ds(0, nt), at, :],
                      xs.at[1, r], xr.at[1, r], (gx - 1, gy, gz))

    def y_up(first, count, t0, tn, send, recv):
        return remote(ext.at[pl.ds(first, count), pl.ds(t0, tn), pl.ds(rows, 8), :],
                      ext.at[pl.ds(first, count), pl.ds(t0, tn), pl.ds(0, 8), :], send, recv,
                      (gx, gy + 1, gz))

    def y_dn(first, count, t0, tn, send, recv):
        return remote(ext.at[pl.ds(first, count), pl.ds(t0, tn), pl.ds(8, 8), :],
                      ext.at[pl.ds(first, count), pl.ds(t0, tn), pl.ds(top, 8), :], send, recv,
                      (gx, gy - 1, gz))

    y_own = (y_up(3, 4, 0, nt, ys.at[0], yr.at[0]), y_dn(3, 4, 0, nt, ys.at[1], yr.at[1]))
    y_edge = (y_up(3, 4, nt, 1, y4s.at[0], y4r.at[0]), y_dn(3, 4, nt, 1, y4s.at[1], y4r.at[1]))
    y_far = [
        (y_up(first, 3, 0, nt + 1, yxs.at[0, s], yxr.at[0, s]), y_dn(first, 3, 0, nt + 1, yxs.at[1, s], yxr.at[1, s]))
        for s, first in ((0, 0), (1, 7))
    ]

    z_own.start()

    @pl.when(has_hi)
    def _():
        x_up(0).start()
        x_up(nr - 1).start()

    @pl.when(has_lo)
    def _():
        x_dn(0).start()
        x_dn(nr - 1).start()

    @pl.when(y_hi)
    def _():
        y_own[0].start()

    @pl.when(y_lo)
    def _():
        y_own[1].start()

    def send_row(r, carry):
        @pl.when(has_hi)
        def _():
            x_up(r).start()

        @pl.when(has_lo)
        def _():
            x_dn(r).start()

        return carry

    first_rows = min(3, nr - 1)
    lax.fori_loop(1, first_rows, send_row, 0)
    for device in ring:
        tell(tok.at[0], device)

    def take_z(first, count, near):
        for p in range(first, first + count):
            if near is None or p == near:
                for c in range(3):
                    zt[p, pl.ds(5 * gz + c, 1), :] = zr[p, c]
            else:
                zt[p, pl.ds(5 * gz + nearest, 1), :] = zr[p, nearest]
        for p in range(first, first + count):
            part = zt[p]
            zero = jnp.zeros_like(part)
            low, high = jnp.where(gz == 0, part, zero), jnp.where(gz == 0, zero, part)
            between = jnp.zeros((LANES - 16, LANES), jnp.float32)
            ext[p, nt, 8:top, :] = jnp.transpose(jnp.concatenate([low, between, high], axis=0))

    z_own.wait_recv()

    @pl.when(has_hi)
    def _():
        z_up[0].start()
        z_up[1].start()

    @pl.when(has_lo)
    def _():
        z_dn[0].start()
        z_dn[1].start()

    lax.fori_loop(first_rows, nr - 1, send_row, 0)
    take_z(3, 4, None)

    @pl.when(has_lo)
    def _():
        z_up[0].wait_recv()
        z_up[1].wait_recv()
        take_z(0, 3, 2)

    @pl.when(has_hi)
    def _():
        z_dn[0].wait_recv()
        z_dn[1].wait_recv()
        take_z(7, 3, 7)

    def arrived(r):
        @pl.when(has_lo)
        def _():
            x_up(r).wait_recv()

        @pl.when(has_hi)
        def _():
            x_dn(r).wait_recv()

    arrived(0)
    arrived(nr - 1)

    for ok, k in ((y_hi, 0), (y_lo, 1)):
        @pl.when(ok)
        def _(k=k):
            y_edge[k].start()

        @pl.when(jnp.logical_and(ok, has_lo))
        def _(k=k):
            y_far[0][k].start()

        @pl.when(jnp.logical_and(ok, has_hi))
        def _(k=k):
            y_far[1][k].start()

    lane = lax.broadcasted_iota(jnp.int32, (8, LANES), 1)

    def columns(tile):
        at = pl.ds(pl.multiple_of(tile * 8, 8), 8)
        sums = []
        for t in range(nt + 1):
            e = [ext[p, t, at, :] for p in range(10)]
            mid = (e[3] + e[4]) + (e[5] + e[6])
            lo2, hi2 = e[2] + e[1], e[7] + e[8]
            sums.append([mid + (lo2 + e[0]), mid + lo2 + e[7], mid + e[2] + hi2, mid + (hi2 + e[9])])
        for x in range(4):
            h = [sums[t][x] for t in range(nt + 1)]
            after = shifted(nt, roll_all(h, 1), 1, lane)
            before = shifted(nt, roll_all(h, -1), -1, lane)
            for t in range(nt):
                c0[x, t, at, :] = h[t]
                d0[x, t, at, :] = after[t] - before[t]
                s0[x, t, at, :] = after[t] + before[t] - 2.0 * h[t]
        for p in range(6):
            f = [ext[2 + p, t, at, :] for t in range(nt + 1)]
            pair = [a + b for a, b in zip(f, shifted(nt + 1, roll_all(f, 1), 1, lane))]
            quad = [a + b for a, b in zip(pair, shifted(nt + 1, roll_all(pair, 2), 2, lane))]
            back = shifted(nt, roll_all(quad, -3), -3, lane)
            for t in range(nt):
                c2[p, t, at, :] = back[t] + (quad[t] - f[t])

    def curve(tile):
        row = tile * 8
        own = pl.ds(pl.multiple_of(row - 8, 8), 8)
        at = pl.ds(pl.multiple_of(row, 8), 8)
        up, dn = pl.ds(row + 1, 8), pl.ds(row - 1, 8)
        col = []
        for p in range(6):
            parts = []
            for t in range(nt + 1):
                v = [ext[2 + p, t, pl.ds(row + k, 8), :] for k in range(-3, 4)]
                parts.append(((v[0] + v[1]) + (v[2] + v[3])) + ((v[4] + v[5]) + v[6]))
            after = shifted(nt, roll_all(parts, 1), 1, lane)
            before = shifted(nt, roll_all(parts, -1), -1, lane)
            col.append((parts, [a - b for a, b in zip(after, before)], [a + b for a, b in zip(after, before)]))
        best = vmax[...]
        for t in range(nt):
            across = pl.ds(t * LANES, LANES)
            for x in range(4):
                o = ori[x, own, across]
                is0, is1 = o == 0, o == 1

                def pick(a, b, c):
                    return jnp.where(is0, a, jnp.where(is1, b, c))

                h0 = c0[x, t, at, :]
                u0, w0 = c0[x, t, up, :], c0[x, t, dn, :]
                h1 = col[x + 1][0][t]
                u1, w1 = col[x + 2][0][t], col[x][0][t]
                h2 = c2[x + 1, t, at, :]
                u2, w2 = c2[x + 2, t, at, :], c2[x, t, at, :]
                b2u, b2w = c2[x + 1, t, up, :], c2[x + 1, t, dn, :]
                twist2 = (c2[x + 2, t, up, :] - c2[x + 2, t, dn, :]) - (c2[x, t, up, :] - c2[x, t, dn, :])
                centre = pick(h0, h1, h2)
                plus, minus = pick(u0, u1, u2), pick(w0, w1, w2)
                slope_a = 0.5 * (plus - minus)
                bend_a = plus + minus - 2.0 * centre
                slope_b = 0.5 * pick(d0[x, t, at, :], col[x + 1][1][t], b2u - b2w)
                bend_b = pick(s0[x, t, at, :], col[x + 1][2][t] - 2.0 * h1, b2u + b2w - 2.0 * h2)
                twist = pick(d0[x, t, up, :] - d0[x, t, dn, :], col[x + 2][1][t] - col[x][1][t], twist2)
                qa, qb = slope_a * slope_a, slope_b * slope_b
                numer = bend_a * (1.0 + qb) + bend_b * (1.0 + qa) - 0.5 * twist * (slope_a * slope_b)
                inv = lax.rsqrt(1.0 + qa + qb)
                kappa = jnp.where(itf[x, own, across] == 1, numer * (inv * inv * inv), 0.0)
                res[x, own, across] = kappa
                best = jnp.maximum(best, jnp.abs(kappa))
        vmax[...] = best

    for ok, k in ((y_lo, 0), (y_hi, 1)):
        @pl.when(ok)
        def _(k=k):
            y_own[k].wait_recv()
            y_edge[k].wait_recv()

        @pl.when(jnp.logical_and(ok, has_lo))
        def _(k=k):
            y_far[0][k].wait_recv()

        @pl.when(jnp.logical_and(ok, has_hi))
        def _(k=k):
            y_far[1][k].wait_recv()

    load_ori.wait()
    load_itf.wait()

    def edges(i, carry):
        columns(i + jnp.where(i >= 2, nr - 2, 0))
        return carry

    lax.fori_loop(0, 4, edges, 0)

    def middle(tile, carry):
        level = tile - 2

        @pl.when(level < tok.shape[0])
        def _():
            pl.semaphore_wait(tok.at[level], len(ring))

        @pl.when(level < tok.shape[0] - 1)
        def _():
            for device in ring:
                tell(tok.at[level + 1], device)

        arrived(tile - 1)
        columns(tile)
        curve(tile - 1)
        return carry

    lax.fori_loop(2, nr, middle, 0)

    def tail(tile, carry):
        curve(tile)
        return carry

    lax.fori_loop(nr - 1, nr + 1, tail, 0)

    r1[me1] = jnp.max(vmax[...], axis=0, keepdims=True)

    def red1(d):
        return remote(r1.at[me1], r1.at[me1], r1s.at[d], r1r.at[d], peer1(d))

    def red2(d):
        return remote(r2.at[me2], r2.at[me2], r2s.at[d], r2r.at[d], peer2(d))

    def recv1(d):
        return remote(r1.at[lax.rem(me1 - d + n1, n1)], r1.at[lax.rem(me1 - d + n1, n1)], r1s.at[d], r1r.at[d], peer1(d))

    def recv2(d):
        return remote(r2.at[lax.rem(me2 - d + n2, n2)], r2.at[lax.rem(me2 - d + n2, n2)], r2s.at[d], r2r.at[d], peer2(d))

    for d in range(1, n1):
        red1(d).start()
    for d in range(1, n1):
        recv1(d).wait_recv()
    r2[me2] = jnp.max(r1[...], axis=0)
    for d in range(1, n2):
        red2(d).start()

    z_own.wait_send()

    def sent_row(r, carry):
        @pl.when(has_hi)
        def _():
            x_up(r).wait_send()

        @pl.when(has_lo)
        def _():
            x_dn(r).wait_send()

        return carry

    lax.fori_loop(0, nr, sent_row, 0)

    @pl.when(has_hi)
    def _():
        z_up[0].wait_send()
        z_up[1].wait_send()

    @pl.when(has_lo)
    def _():
        z_dn[0].wait_send()
        z_dn[1].wait_send()

    for ok, k in ((y_hi, 0), (y_lo, 1)):
        @pl.when(ok)
        def _(k=k):
            y_own[k].wait_send()
            y_edge[k].wait_send()

        @pl.when(jnp.logical_and(ok, has_lo))
        def _(k=k):
            y_far[0][k].wait_send()

        @pl.when(jnp.logical_and(ok, has_hi))
        def _(k=k):
            y_far[1][k].wait_send()

    for d in range(1, n1):
        red1(d).wait_send()
    for d in range(1, n2):
        recv2(d).wait_recv()
    peak_ref[...] = jnp.max(r2[...], axis=0)
    for d in range(1, n2):
        red2(d).wait_send()


def settle(res, peak, out, peak_out, top, sems):
    copies = [pltpu.make_async_copy(res.at[p], out.at[p], sems.at[p]) for p in range(res.shape[0])]
    for copy in copies:
        copy.start()
    top[0, 0] = jnp.max(peak[...])
    last = pltpu.make_async_copy(top, peak_out, sems.at[res.shape[0]])
    last.start()
    last.wait()
    for copy in copies:
        copy.wait()


def block(sizes, fraction, orientation, interface):
    planes, rows, lanes = fraction.shape
    ngx, ngy, ngz, zhi = sizes
    nt, nr = lanes // LANES, rows // 8
    n1, n2 = zhi * ngz, (ngx // zhi) * ngy
    hops = ngy // 4 + ngx // zhi // 2 + 1
    dma = pltpu.SemaphoreType.DMA
    f32 = jnp.float32
    curvature, peak = pl.pallas_call(
        functools.partial(kernel, sizes),
        out_shape=(
            jax.ShapeDtypeStruct(fraction.shape, f32),
            jax.ShapeDtypeStruct((1, LANES), f32),
        ),
        in_specs=[pl.BlockSpec(memory_space=pl.ANY)] * 3,
        out_specs=(pl.BlockSpec(memory_space=pltpu.VMEM), pl.BlockSpec(memory_space=pltpu.VMEM)),
        scratch_shapes=[
            pltpu.VMEM((10, nt + 1, rows + 16, LANES), f32),
            pltpu.VMEM((4, nt, rows + 16, LANES), f32),
            pltpu.VMEM((4, nt, rows + 16, LANES), f32),
            pltpu.VMEM((4, nt, rows + 16, LANES), f32),
            pltpu.VMEM((6, nt, rows + 16, LANES), f32),
            pltpu.VMEM((planes, rows, lanes), jnp.int32),
            pltpu.VMEM((planes, rows, lanes), jnp.int32),
            pltpu.VMEM((4, 3, 1, LANES), f32),
            pltpu.VMEM((10, 3, 1, LANES), f32),
            pltpu.VMEM((10, 8, LANES), f32),
            pltpu.VMEM((8, LANES), f32),
            pltpu.VMEM((n1, 1, LANES), f32),
            pltpu.VMEM((n2, 1, LANES), f32),
            dma((nt + 2,)),
            dma((2, nr)), dma((2, nr)),
            dma((2,)), dma((2,)),
            dma((2,)), dma((2,)),
            dma((2, 2)), dma((2, 2)),
            dma((5,)), dma((5,)),
            dma((n1,)), dma((n1,)),
            dma((n2,)), dma((n2,)),
            pltpu.SemaphoreType.REGULAR((hops - 1,)),
        ],
        compiler_params=pltpu.CompilerParams(
            collective_id=0, has_side_effects=True, vmem_limit_bytes=55000000
        ),
    )(fraction, orientation, interface)
    curvature, peak = pl.pallas_call(
        settle,
        out_shape=(
            jax.ShapeDtypeStruct(fraction.shape, f32),
            jax.ShapeDtypeStruct((1, 1), f32),
        ),
        in_specs=[pl.BlockSpec(memory_space=pltpu.VMEM), pl.BlockSpec(memory_space=pltpu.VMEM)],
        out_specs=(pl.BlockSpec(memory_space=pl.ANY),) * 2,
        scratch_shapes=[pltpu.SMEM((1, 1), f32), dma((planes + 1,))], compiler_params=pltpu.CompilerParams(vmem_limit_bytes=1048576 * 2),
    )(curvature, peak)
    return curvature, peak.reshape(())


def solution(mesh):
    sizes = (mesh.shape["gx"], mesh.shape["gy"], mesh.shape["gz"], min(Z_HI, mesh.shape["gx"]))
    spec = P("gx", "gy", "gz")
    return jax.shard_map(
        functools.partial(block, sizes), mesh=mesh, in_specs=(spec,) * 3, out_specs=(spec, P()), check_vma=False
    )
```

```python
import functools

import jax
import jax.numpy as jnp
from jax import lax
from jax.experimental import pallas as pl
from jax.experimental.pallas import tpu as pltpu
from jax.sharding import PartitionSpec as P

MESH = pl.DeviceIdType.MESH
LANES = 128
Z_HI = 4


def shifted(tiles, rolled, shift, lane):
    count = len(rolled)
    out = []
    for t in range(tiles):
        if shift > 0:
            out.append(jnp.where(lane >= LANES - shift, rolled[(t + 1) % count], rolled[t]))
        else:
            out.append(jnp.where(lane < -shift, rolled[(t - 1) % count], rolled[t]))
    return out


def roll_all(tiles, shift):
    return [pltpu.roll(x, (-shift) % LANES, x.ndim - 1) for x in tiles]


def kernel(
    sizes, f_hbm, ori_hbm, itf_hbm, res, peak_ref,
    ext, c0, d0, s0, c2, ori, itf, zs, zr, zt, vmax, r1, r2,
    load_sem, xs, xr, ys, yr, y4s, y4r, yxs, yxr, zss, zrs, r1s, r1r, r2s, r2r, tok,
):
    ngx, ngy, ngz, zhi = sizes
    gx, gy, gz = lax.axis_index("gx"), lax.axis_index("gy"), lax.axis_index("gz")
    other = 1 - gz
    planes, rows, lanes = f_hbm.shape
    nt = lanes // LANES
    nr = rows // 8
    has_lo, has_hi = gx > 0, gx < ngx - 1
    y_lo, y_hi = gy > 0, gy < ngy - 1
    top = 8 + rows

    loads = [
        pltpu.make_async_copy(
            f_hbm.at[:, :, pl.ds(t * LANES, LANES)], ext.at[pl.ds(3, 4), t, pl.ds(8, rows), :],
            load_sem.at[t])
        for t in range(nt)
    ]
    load_ori = pltpu.make_async_copy(ori_hbm, ori, load_sem.at[nt])
    load_itf = pltpu.make_async_copy(itf_hbm, itf, load_sem.at[nt + 1])
    for copy in loads:
        copy.start()
    load_ori.start()
    load_itf.start()

    ny, nx = ngx // zhi, ngy // 2
    y_at, z_at = gx // zhi, gx % zhi
    x_at, core = gy // 2, lax.rem(gy, 2)
    n1, n2 = ny * ngy, zhi * ngz
    me1, me2 = y_at * ngy + gy, z_at * ngz + gz

    def around(d, n):
        return min(d, n - d)

    steps1 = [(dy, dx, dc) for dy in range(ny) for dx in range(nx) for dc in range(2)][1:]
    steps1.sort(key=lambda d: (-around(d[0], ny) - around(d[1], nx), -d[2]))
    steps2 = sorted(range(1, n2), key=lambda d: -around(d, n2))

    def peer1(step, sign):
        dy, dx, dc = step
        y = lax.rem(y_at + sign * dy + ny, ny)
        x = lax.rem(x_at + sign * dx + nx, nx)
        return y, x * 2 + (1 - core if dc else core)

    def peer2(d, sign):
        return lax.rem(me2 + sign * d + n2, n2)

    def steps(n):
        return (1, n - 1) if n > 2 else (1,) * (n - 1)

    ring = [(y_at * zhi + lax.rem(z_at + d, zhi), gy, gz) for d in steps(zhi)]
    ring += [(lax.rem(y_at + d, ny) * zhi + z_at, gy, gz) for d in steps(ny)]
    ring += [(gx, lax.rem(x_at + d, nx) * 2 + core, gz) for d in steps(nx)]
    ring += [(gx, gy, other), (gx, gy + 1 - 2 * core, gz)]
    barrier = pltpu.get_barrier_semaphore()

    def tell(semaphore, device):
        pl.semaphore_signal(semaphore, inc=1, device_id=device, device_id_type=MESH)

    extra = (
        (jnp.logical_and(has_hi, z_at == zhi - 1), (gx + 1, gy, gz)),
        (jnp.logical_and(has_lo, z_at == 0), (gx - 1, gy, gz)),
        (jnp.logical_and(y_hi, core == 1), (gx, gy + 1, gz)),
        (jnp.logical_and(y_lo, core == 0), (gx, gy - 1, gz)),
    )
    for ok, device in extra:
        @pl.when(ok)
        def _(device=device):
            tell(barrier, device)

    for device in ring:
        tell(barrier, device)
    greeted = len(ring)
    for ok, _ in extra:
        greeted = greeted + jnp.where(ok, 1, 0)

    @pl.when(jnp.logical_not(has_lo))
    def _():
        ext[0:3] = jnp.zeros((3, nt + 1, rows + 16, LANES), jnp.float32)

    @pl.when(jnp.logical_not(has_hi))
    def _():
        ext[7:10] = jnp.zeros((3, nt + 1, rows + 16, LANES), jnp.float32)

    @pl.when(jnp.logical_not(y_lo))
    def _():
        ext[:, :, 0:8] = jnp.zeros((10, nt + 1, 8, LANES), jnp.float32)

    @pl.when(jnp.logical_not(y_hi))
    def _():
        ext[:, :, top:top + 8] = jnp.zeros((10, nt + 1, 8, LANES), jnp.float32)

    for copy in loads:
        copy.wait()

    edge = jnp.where(gz == 0, nt - 1, 0)
    for p in range(4):
        turned = jnp.transpose(ext[3 + p, edge, 8:top, :])
        part = jnp.where(gz == 0, turned[LANES - 3:LANES], turned[0:3])
        for c in range(3):
            zs[p, c] = part[c:c + 1]
    zt[...] = jnp.zeros_like(zt)
    vmax[...] = jnp.zeros_like(vmax)

    pl.semaphore_wait(barrier, greeted)

    def remote(src, dst, send, recv, device):
        return pltpu.make_async_remote_copy(
            src_ref=src, dst_ref=dst, send_sem=send, recv_sem=recv, device_id=device,
            device_id_type=MESH)

    nearest = 2 * gz
    z_own = remote(zs, zr.at[pl.ds(3, 4)], zss.at[0], zrs.at[0], (gx, gy, other))
    z_up = (
        remote(zr.at[6], zr.at[2], zss.at[1], zrs.at[1], (gx + 1, gy, gz)),
        remote(zr.at[pl.ds(4, 2), nearest], zr.at[pl.ds(0, 2), nearest], zss.at[2], zrs.at[2], (gx + 1, gy, gz)),
    )
    z_dn = (
        remote(zr.at[3], zr.at[7], zss.at[3], zrs.at[3], (gx - 1, gy, gz)),
        remote(zr.at[pl.ds(4, 2), nearest], zr.at[pl.ds(8, 2), nearest], zss.at[4], zrs.at[4], (gx - 1, gy, gz)),
    )

    def x_up(r):
        at = pl.ds(pl.multiple_of(8 + r * 8, 8), 8)
        return remote(ext.at[pl.ds(4, 3), pl.ds(0, nt), at, :], ext.at[pl.ds(0, 3), pl.ds(0, nt), at, :],
                      xs.at[0, r], xr.at[0, r], (gx + 1, gy, gz))

    def x_dn(r):
        at = pl.ds(pl.multiple_of(8 + r * 8, 8), 8)
        return remote(ext.at[pl.ds(3, 3), pl.ds(0, nt), at, :], ext.at[pl.ds(7, 3), pl.ds(0, nt), at, :],
                      xs.at[1, r], xr.at[1, r], (gx - 1, gy, gz))

    def y_up(first, count, t0, tn, send, recv):
        return remote(ext.at[pl.ds(first, count), pl.ds(t0, tn), pl.ds(rows, 8), :],
                      ext.at[pl.ds(first, count), pl.ds(t0, tn), pl.ds(0, 8), :], send, recv,
                      (gx, gy + 1, gz))

    def y_dn(first, count, t0, tn, send, recv):
        return remote(ext.at[pl.ds(first, count), pl.ds(t0, tn), pl.ds(8, 8), :],
                      ext.at[pl.ds(first, count), pl.ds(t0, tn), pl.ds(top, 8), :], send, recv,
                      (gx, gy - 1, gz))

    y_own = (y_up(3, 4, 0, nt, ys.at[0], yr.at[0]), y_dn(3, 4, 0, nt, ys.at[1], yr.at[1]))
    y_edge = (y_up(3, 4, nt, 1, y4s.at[0], y4r.at[0]), y_dn(3, 4, nt, 1, y4s.at[1], y4r.at[1]))
    y_far = [
        (y_up(first, 3, 0, nt + 1, yxs.at[0, s], yxr.at[0, s]), y_dn(first, 3, 0, nt + 1, yxs.at[1, s], yxr.at[1, s]))
        for s, first in ((0, 0), (1, 7))
    ]

    z_own.start()

    @pl.when(has_hi)
    def _():
        x_up(0).start()
        x_up(nr - 1).start()

    @pl.when(has_lo)
    def _():
        x_dn(0).start()
        x_dn(nr - 1).start()

    @pl.when(y_hi)
    def _():
        y_own[0].start()

    @pl.when(y_lo)
    def _():
        y_own[1].start()

    def send_row(r, carry):
        @pl.when(has_hi)
        def _():
            x_up(r).start()

        @pl.when(has_lo)
        def _():
            x_dn(r).start()

        return carry

    first_rows = 1
    lax.fori_loop(1, first_rows, send_row, 0)
    for device in ring:
        tell(tok.at[0], device)

    def take_z(first, count, near):
        for p in range(first, first + count):
            if near is None or p == near:
                for c in range(3):
                    zt[p, pl.ds(5 * gz + c, 1), :] = zr[p, c]
            else:
                zt[p, pl.ds(5 * gz + nearest, 1), :] = zr[p, nearest]
        for p in range(first, first + count):
            part = zt[p]
            zero = jnp.zeros_like(part)
            low, high = jnp.where(gz == 0, part, zero), jnp.where(gz == 0, zero, part)
            between = jnp.zeros((LANES - 16, LANES), jnp.float32)
            ext[p, nt, 8:top, :] = jnp.transpose(jnp.concatenate([low, between, high], axis=0))

    z_own.wait_recv()

    @pl.when(has_hi)
    def _():
        z_up[0].start()
        z_up[1].start()

    @pl.when(has_lo)
    def _():
        z_dn[0].start()
        z_dn[1].start()

    lax.fori_loop(first_rows, nr - 1, send_row, 0)
    take_z(3, 4, None)

    @pl.when(has_lo)
    def _():
        z_up[0].wait_recv()
        z_up[1].wait_recv()
        take_z(0, 3, 2)

    @pl.when(has_hi)
    def _():
        z_dn[0].wait_recv()
        z_dn[1].wait_recv()
        take_z(7, 3, 7)

    def arrived(r):
        @pl.when(has_lo)
        def _():
            x_up(r).wait_recv()

        @pl.when(has_hi)
        def _():
            x_dn(r).wait_recv()

    arrived(0)
    arrived(nr - 1)

    for ok, k in ((y_hi, 0), (y_lo, 1)):
        @pl.when(ok)
        def _(k=k):
            y_edge[k].start()

        @pl.when(jnp.logical_and(ok, has_lo))
        def _(k=k):
            y_far[0][k].start()

        @pl.when(jnp.logical_and(ok, has_hi))
        def _(k=k):
            y_far[1][k].start()

    lane = lax.broadcasted_iota(jnp.int32, (8, LANES), 1)

    def columns(tile):
        at = pl.ds(pl.multiple_of(tile * 8, 8), 8)
        sums = []
        for t in range(nt + 1):
            e = [ext[p, t, at, :] for p in range(10)]
            mid = (e[3] + e[4]) + (e[5] + e[6])
            lo2, hi2 = e[2] + e[1], e[7] + e[8]
            sums.append([mid + (lo2 + e[0]), mid + lo2 + e[7], mid + e[2] + hi2, mid + (hi2 + e[9])])
        for x in range(4):
            h = [sums[t][x] for t in range(nt + 1)]
            after = shifted(nt, roll_all(h, 1), 1, lane)
            before = shifted(nt, roll_all(h, -1), -1, lane)
            for t in range(nt):
                c0[x, t, at, :] = h[t]
                d0[x, t, at, :] = after[t] - before[t]
                s0[x, t, at, :] = after[t] + before[t] - 2.0 * h[t]
        for p in range(6):
            f = [ext[2 + p, t, at, :] for t in range(nt + 1)]
            pair = [a + b for a, b in zip(f, shifted(nt + 1, roll_all(f, 1), 1, lane))]
            quad = [a + b for a, b in zip(pair, shifted(nt + 1, roll_all(pair, 2), 2, lane))]
            back = shifted(nt, roll_all(quad, -3), -3, lane)
            for t in range(nt):
                c2[p, t, at, :] = back[t] + (quad[t] - f[t])

    def curve(tile):
        row = tile * 8
        own = pl.ds(pl.multiple_of(row - 8, 8), 8)
        at = pl.ds(pl.multiple_of(row, 8), 8)
        up, dn = pl.ds(row + 1, 8), pl.ds(row - 1, 8)
        col = []
        for p in range(6):
            parts = []
            for t in range(nt + 1):
                v = [ext[2 + p, t, pl.ds(row + k, 8), :] for k in range(-3, 4)]
                parts.append(((v[0] + v[1]) + (v[2] + v[3])) + ((v[4] + v[5]) + v[6]))
            after = shifted(nt, roll_all(parts, 1), 1, lane)
            before = shifted(nt, roll_all(parts, -1), -1, lane)
            col.append((parts, [a - b for a, b in zip(after, before)], [a + b for a, b in zip(after, before)]))
        best = vmax[...]
        for t in range(nt):
            across = pl.ds(t * LANES, LANES)
            for x in range(4):
                o = ori[x, own, across]
                is0, is1 = o == 0, o == 1

                def pick(a, b, c):
                    return jnp.where(is0, a, jnp.where(is1, b, c))

                h0 = c0[x, t, at, :]
                u0, w0 = c0[x, t, up, :], c0[x, t, dn, :]
                h1 = col[x + 1][0][t]
                u1, w1 = col[x + 2][0][t], col[x][0][t]
                h2 = c2[x + 1, t, at, :]
                u2, w2 = c2[x + 2, t, at, :], c2[x, t, at, :]
                b2u, b2w = c2[x + 1, t, up, :], c2[x + 1, t, dn, :]
                twist2 = (c2[x + 2, t, up, :] - c2[x + 2, t, dn, :]) - (c2[x, t, up, :] - c2[x, t, dn, :])
                centre = pick(h0, h1, h2)
                plus, minus = pick(u0, u1, u2), pick(w0, w1, w2)
                slope_a = 0.5 * (plus - minus)
                bend_a = plus + minus - 2.0 * centre
                slope_b = 0.5 * pick(d0[x, t, at, :], col[x + 1][1][t], b2u - b2w)
                bend_b = pick(s0[x, t, at, :], col[x + 1][2][t] - 2.0 * h1, b2u + b2w - 2.0 * h2)
                twist = pick(d0[x, t, up, :] - d0[x, t, dn, :], col[x + 2][1][t] - col[x][1][t], twist2)
                qa, qb = slope_a * slope_a, slope_b * slope_b
                numer = bend_a * (1.0 + qb) + bend_b * (1.0 + qa) - 0.5 * twist * (slope_a * slope_b)
                inv = lax.rsqrt(1.0 + qa + qb)
                kappa = jnp.where(itf[x, own, across] == 1, numer * (inv * inv * inv), 0.0)
                res[x, own, across] = kappa
                best = jnp.maximum(best, jnp.abs(kappa))
        vmax[...] = best

    for ok, k in ((y_lo, 0), (y_hi, 1)):
        @pl.when(ok)
        def _(k=k):
            y_own[k].wait_recv()
            y_edge[k].wait_recv()

        @pl.when(jnp.logical_and(ok, has_lo))
        def _(k=k):
            y_far[0][k].wait_recv()

        @pl.when(jnp.logical_and(ok, has_hi))
        def _(k=k):
            y_far[1][k].wait_recv()

    load_ori.wait()
    load_itf.wait()

    def edges(i, carry):
        columns(i + jnp.where(i >= 2, nr - 2, 0))
        return carry

    lax.fori_loop(0, 4, edges, 0)

    def middle(tile, carry):
        level = tile - 2

        @pl.when(level < tok.shape[0])
        def _():
            pl.semaphore_wait(tok.at[level], len(ring))

        @pl.when(level < tok.shape[0] - 1)
        def _():
            for device in ring:
                tell(tok.at[level + 1], device)

        arrived(tile - 1)
        columns(tile)
        curve(tile - 1)
        return carry

    lax.fori_loop(2, nr, middle, 0)

    def tail(tile, carry):
        curve(tile)
        return carry

    lax.fori_loop(nr - 1, nr + 1, tail, 0)

    r1[me1] = jnp.max(vmax[...], axis=0, keepdims=True)

    def red1(k, sign=1):
        y, at = peer1(steps1[k], sign)
        slot = me1 if sign > 0 else y * ngy + at
        return remote(r1.at[slot], r1.at[slot], r1s.at[k], r1r.at[k], (y * zhi + z_at, at, gz))

    def red2(k, sign=1):
        i = peer2(steps2[k], sign)
        slot = me2 if sign > 0 else i
        return remote(r2.at[slot], r2.at[slot], r2s.at[k], r2r.at[k], (y_at * zhi + i // ngz, gy, lax.rem(i, ngz)))

    for d in range(n1 - 1):
        red1(d).start()
    for d in range(n1 - 1):
        red1(d, -1).wait_recv()
    r2[me2] = jnp.max(r1[...], axis=0)
    for d in range(n2 - 1):
        red2(d).start()

    z_own.wait_send()

    def sent_row(r, carry):
        @pl.when(has_hi)
        def _():
            x_up(r).wait_send()

        @pl.when(has_lo)
        def _():
            x_dn(r).wait_send()

        return carry

    lax.fori_loop(0, nr, sent_row, 0)

    @pl.when(has_hi)
    def _():
        z_up[0].wait_send()
        z_up[1].wait_send()

    @pl.when(has_lo)
    def _():
        z_dn[0].wait_send()
        z_dn[1].wait_send()

    for ok, k in ((y_hi, 0), (y_lo, 1)):
        @pl.when(ok)
        def _(k=k):
            y_own[k].wait_send()
            y_edge[k].wait_send()

        @pl.when(jnp.logical_and(ok, has_lo))
        def _(k=k):
            y_far[0][k].wait_send()

        @pl.when(jnp.logical_and(ok, has_hi))
        def _(k=k):
            y_far[1][k].wait_send()

    for d in range(n1 - 1):
        red1(d).wait_send()
    for d in range(n2 - 1):
        red2(d, -1).wait_recv()
    peak_ref[...] = jnp.max(r2[...], axis=0)
    for d in range(n2 - 1):
        red2(d).wait_send()


def settle(res, peak, out, peak_out, top, sems):
    copies = [pltpu.make_async_copy(res.at[p], out.at[p], sems.at[p]) for p in range(res.shape[0])]
    for copy in copies:
        copy.start()
    top[0, 0] = jnp.max(peak[...])
    last = pltpu.make_async_copy(top, peak_out, sems.at[res.shape[0]])
    last.start()
    last.wait()
    for copy in copies:
        copy.wait()


def block(sizes, fraction, orientation, interface):
    planes, rows, lanes = fraction.shape
    ngx, ngy, ngz, zhi = sizes
    nt, nr = lanes // LANES, rows // 8
    n1, n2 = (ngx // zhi) * ngy, zhi * ngz
    hops = ngy // 4 + ngx // zhi // 2 + 1
    dma = pltpu.SemaphoreType.DMA
    f32 = jnp.float32
    curvature, peak = pl.pallas_call(
        functools.partial(kernel, sizes),
        out_shape=(
            jax.ShapeDtypeStruct(fraction.shape, f32),
            jax.ShapeDtypeStruct((1, LANES), f32),
        ),
        in_specs=[pl.BlockSpec(memory_space=pl.ANY)] * 3,
        out_specs=(pl.BlockSpec(memory_space=pltpu.VMEM), pl.BlockSpec(memory_space=pltpu.VMEM)),
        scratch_shapes=[
            pltpu.VMEM((10, nt + 1, rows + 16, LANES), f32),
            pltpu.VMEM((4, nt, rows + 16, LANES), f32),
            pltpu.VMEM((4, nt, rows + 16, LANES), f32),
            pltpu.VMEM((4, nt, rows + 16, LANES), f32),
            pltpu.VMEM((6, nt, rows + 16, LANES), f32),
            pltpu.VMEM((planes, rows, lanes), jnp.int32),
            pltpu.VMEM((planes, rows, lanes), jnp.int32),
            pltpu.VMEM((4, 3, 1, LANES), f32),
            pltpu.VMEM((10, 3, 1, LANES), f32),
            pltpu.VMEM((10, 8, LANES), f32),
            pltpu.VMEM((8, LANES), f32),
            pltpu.VMEM((n1, 1, LANES), f32),
            pltpu.VMEM((n2, 1, LANES), f32),
            dma((nt + 2,)),
            dma((2, nr)), dma((2, nr)),
            dma((2,)), dma((2,)),
            dma((2,)), dma((2,)),
            dma((2, 2)), dma((2, 2)),
            dma((5,)), dma((5,)),
            dma((n1,)), dma((n1,)),
            dma((n2,)), dma((n2,)),
            pltpu.SemaphoreType.REGULAR((hops - 1,)),
        ],
        compiler_params=pltpu.CompilerParams(
            collective_id=0, has_side_effects=True, vmem_limit_bytes=55000000
        ),
    )(fraction, orientation, interface)
    curvature, peak = pl.pallas_call(
        settle,
        out_shape=(
            jax.ShapeDtypeStruct(fraction.shape, f32),
            jax.ShapeDtypeStruct((1, 1), f32),
        ),
        in_specs=[pl.BlockSpec(memory_space=pltpu.VMEM), pl.BlockSpec(memory_space=pltpu.VMEM)],
        out_specs=(pl.BlockSpec(memory_space=pl.ANY),) * 2,
        scratch_shapes=[pltpu.SMEM((1, 1), f32), dma((planes + 1,))], compiler_params=pltpu.CompilerParams(vmem_limit_bytes=1048576 * 2),
    )(curvature, peak)
    return curvature, peak.reshape(())


def solution(mesh):
    sizes = (mesh.shape["gx"], mesh.shape["gy"], mesh.shape["gz"], min(Z_HI, mesh.shape["gx"]))
    spec = P("gx", "gy", "gz")
    return jax.shard_map(
        functools.partial(block, sizes), mesh=mesh, in_specs=(spec,) * 3, out_specs=(spec, P()), check_vma=False
    )
```

```python
import functools

import jax
import jax.numpy as jnp
from jax import lax
from jax.experimental import pallas as pl
from jax.experimental.pallas import tpu as pltpu
from jax.sharding import PartitionSpec as P

MESH = pl.DeviceIdType.MESH
LANES = 128
Z_HI = 4


def shifted(tiles, rolled, shift, lane):
    count = len(rolled)
    out = []
    for t in range(tiles):
        if shift > 0:
            out.append(jnp.where(lane >= LANES - shift, rolled[(t + 1) % count], rolled[t]))
        else:
            out.append(jnp.where(lane < -shift, rolled[(t - 1) % count], rolled[t]))
    return out


def roll_all(tiles, shift):
    return [pltpu.roll(x, (-shift) % LANES, x.ndim - 1) for x in tiles]


def kernel(
    sizes, f_hbm, ori_hbm, itf_hbm, res, peak_ref,
    ext, c0, d0, s0, c2, ori, itf, zs, zr, zt, vmax, r1, r2,
    load_sem, xs, xr, ys, yr, y4s, y4r, yxs, yxr, zss, zrs, r1s, r1r, r2s, r2r, tok,
):
    ngx, ngy, ngz, zhi = sizes
    gx, gy, gz = lax.axis_index("gx"), lax.axis_index("gy"), lax.axis_index("gz")
    other = 1 - gz
    planes, rows, lanes = f_hbm.shape
    nt = lanes // LANES
    nr = rows // 8
    has_lo, has_hi = gx > 0, gx < ngx - 1
    y_lo, y_hi = gy > 0, gy < ngy - 1
    top = 8 + rows

    loads = [
        pltpu.make_async_copy(
            f_hbm.at[:, :, pl.ds(t * LANES, LANES)], ext.at[pl.ds(3, 4), t, pl.ds(8, rows), :],
            load_sem.at[t])
        for t in range(nt)
    ]
    load_ori = pltpu.make_async_copy(ori_hbm, ori, load_sem.at[nt])
    load_itf = pltpu.make_async_copy(itf_hbm, itf, load_sem.at[nt + 1])
    ny, nx = ngx // zhi, ngy // 2
    y_at, z_at = gx // zhi, gx % zhi
    x_at, core = gy // 2, lax.rem(gy, 2)
    n1, n2 = ny * ngy, zhi * ngz
    me1, me2 = y_at * ngy + gy, z_at * ngz + gz

    def around(d, n):
        return min(d, n - d)

    steps1 = [(dy, dx, dc) for dy in range(ny) for dx in range(nx) for dc in range(2)][1:]
    steps1.sort(key=lambda d: (-around(d[0], ny) - around(d[1], nx), -d[2]))
    steps2 = sorted(range(1, n2), key=lambda d: -around(d, n2))

    def peer1(step, sign):
        dy, dx, dc = step
        y = lax.rem(y_at + sign * dy + ny, ny)
        x = lax.rem(x_at + sign * dx + nx, nx)
        return y, x * 2 + (1 - core if dc else core)

    def peer2(d, sign):
        return lax.rem(me2 + sign * d + n2, n2)

    def steps(n):
        return (1, n - 1) if n > 2 else (1,) * (n - 1)

    ring = [(y_at * zhi + lax.rem(z_at + d, zhi), gy, gz) for d in steps(zhi)]
    ring += [(lax.rem(y_at + d, ny) * zhi + z_at, gy, gz) for d in steps(ny)]
    ring += [(gx, lax.rem(x_at + d, nx) * 2 + core, gz) for d in steps(nx)]
    ring += [(gx, gy, other), (gx, gy + 1 - 2 * core, gz)]
    barrier = pltpu.get_barrier_semaphore()

    def tell(semaphore, device):
        pl.semaphore_signal(semaphore, inc=1, device_id=device, device_id_type=MESH)

    extra = (
        (jnp.logical_and(has_hi, z_at == zhi - 1), (gx + 1, gy, gz)),
        (jnp.logical_and(has_lo, z_at == 0), (gx - 1, gy, gz)),
        (jnp.logical_and(y_hi, core == 1), (gx, gy + 1, gz)),
        (jnp.logical_and(y_lo, core == 0), (gx, gy - 1, gz)),
    )
    for ok, device in extra:
        @pl.when(ok)
        def _(device=device):
            tell(barrier, device)

    for device in ring:
        tell(barrier, device)
    for copy in loads:
        copy.start()
    load_ori.start()
    load_itf.start()
    greeted = len(ring)
    for ok, _ in extra:
        greeted = greeted + jnp.where(ok, 1, 0)

    @pl.when(jnp.logical_not(has_lo))
    def _():
        ext[0:3] = jnp.zeros((3, nt + 1, rows + 16, LANES), jnp.float32)

    @pl.when(jnp.logical_not(has_hi))
    def _():
        ext[7:10] = jnp.zeros((3, nt + 1, rows + 16, LANES), jnp.float32)

    @pl.when(jnp.logical_not(y_lo))
    def _():
        ext[:, :, 0:8] = jnp.zeros((10, nt + 1, 8, LANES), jnp.float32)

    @pl.when(jnp.logical_not(y_hi))
    def _():
        ext[:, :, top:top + 8] = jnp.zeros((10, nt + 1, 8, LANES), jnp.float32)

    for copy in loads:
        copy.wait()

    edge = jnp.where(gz == 0, nt - 1, 0)
    for p in range(4):
        turned = jnp.transpose(ext[3 + p, edge, 8:top, :])
        part = jnp.where(gz == 0, turned[LANES - 3:LANES], turned[0:3])
        for c in range(3):
            zs[p, c] = part[c:c + 1]
    zt[...] = jnp.zeros_like(zt)
    vmax[...] = jnp.zeros_like(vmax)

    pl.semaphore_wait(barrier, greeted)

    def remote(src, dst, send, recv, device):
        return pltpu.make_async_remote_copy(
            src_ref=src, dst_ref=dst, send_sem=send, recv_sem=recv, device_id=device,
            device_id_type=MESH)

    nearest = 2 * gz
    z_own = remote(zs, zr.at[pl.ds(3, 4)], zss.at[0], zrs.at[0], (gx, gy, other))
    z_up = (
        remote(zr.at[6], zr.at[2], zss.at[1], zrs.at[1], (gx + 1, gy, gz)),
        remote(zr.at[pl.ds(4, 2), nearest], zr.at[pl.ds(0, 2), nearest], zss.at[2], zrs.at[2], (gx + 1, gy, gz)),
    )
    z_dn = (
        remote(zr.at[3], zr.at[7], zss.at[3], zrs.at[3], (gx - 1, gy, gz)),
        remote(zr.at[pl.ds(4, 2), nearest], zr.at[pl.ds(8, 2), nearest], zss.at[4], zrs.at[4], (gx - 1, gy, gz)),
    )

    def x_up(r):
        at = pl.ds(pl.multiple_of(8 + r * 8, 8), 8)
        return remote(ext.at[pl.ds(4, 3), pl.ds(0, nt), at, :], ext.at[pl.ds(0, 3), pl.ds(0, nt), at, :],
                      xs.at[0, r], xr.at[0, r], (gx + 1, gy, gz))

    def x_dn(r):
        at = pl.ds(pl.multiple_of(8 + r * 8, 8), 8)
        return remote(ext.at[pl.ds(3, 3), pl.ds(0, nt), at, :], ext.at[pl.ds(7, 3), pl.ds(0, nt), at, :],
                      xs.at[1, r], xr.at[1, r], (gx - 1, gy, gz))

    def y_up(first, count, t0, tn, send, recv):
        return remote(ext.at[pl.ds(first, count), pl.ds(t0, tn), pl.ds(rows, 8), :],
                      ext.at[pl.ds(first, count), pl.ds(t0, tn), pl.ds(0, 8), :], send, recv,
                      (gx, gy + 1, gz))

    def y_dn(first, count, t0, tn, send, recv):
        return remote(ext.at[pl.ds(first, count), pl.ds(t0, tn), pl.ds(8, 8), :],
                      ext.at[pl.ds(first, count), pl.ds(t0, tn), pl.ds(top, 8), :], send, recv,
                      (gx, gy - 1, gz))

    y_own = (y_up(3, 4, 0, nt, ys.at[0], yr.at[0]), y_dn(3, 4, 0, nt, ys.at[1], yr.at[1]))
    y_edge = (y_up(3, 4, nt, 1, y4s.at[0], y4r.at[0]), y_dn(3, 4, nt, 1, y4s.at[1], y4r.at[1]))
    y_far = [
        (y_up(first, 3, 0, nt + 1, yxs.at[0, s], yxr.at[0, s]), y_dn(first, 3, 0, nt + 1, yxs.at[1, s], yxr.at[1, s]))
        for s, first in ((0, 0), (1, 7))
    ]

    z_own.start()

    @pl.when(has_hi)
    def _():
        x_up(0).start()
        x_up(nr - 1).start()

    @pl.when(has_lo)
    def _():
        x_dn(0).start()
        x_dn(nr - 1).start()

    @pl.when(y_hi)
    def _():
        y_own[0].start()

    @pl.when(y_lo)
    def _():
        y_own[1].start()

    def send_row(r, carry):
        @pl.when(has_hi)
        def _():
            x_up(r).start()

        @pl.when(has_lo)
        def _():
            x_dn(r).start()

        return carry

    first_rows = 1
    lax.fori_loop(1, first_rows, send_row, 0)
    def pass_on(level):
        if level > 0 and level <= tok.shape[0]:
            pl.semaphore_wait(tok.at[level - 1], len(ring))
        if level < tok.shape[0]:
            for device in ring:
                tell(tok.at[level], device)

    pass_on(0)

    def take_z(first, count, near):
        for p in range(first, first + count):
            if near is None or p == near:
                for c in range(3):
                    zt[p, pl.ds(5 * gz + c, 1), :] = zr[p, c]
            else:
                zt[p, pl.ds(5 * gz + nearest, 1), :] = zr[p, nearest]
        for p in range(first, first + count):
            part = zt[p]
            zero = jnp.zeros_like(part)
            low, high = jnp.where(gz == 0, part, zero), jnp.where(gz == 0, zero, part)
            between = jnp.zeros((LANES - 16, LANES), jnp.float32)
            ext[p, nt, 8:top, :] = jnp.transpose(jnp.concatenate([low, between, high], axis=0))

    z_own.wait_recv()

    @pl.when(has_hi)
    def _():
        z_up[0].start()
        z_up[1].start()

    @pl.when(has_lo)
    def _():
        z_dn[0].start()
        z_dn[1].start()

    lax.fori_loop(first_rows, nr - 1, send_row, 0)
    take_z(3, 4, None)
    pass_on(1)

    @pl.when(has_lo)
    def _():
        z_up[0].wait_recv()
        z_up[1].wait_recv()
        take_z(0, 3, 2)

    @pl.when(has_hi)
    def _():
        z_dn[0].wait_recv()
        z_dn[1].wait_recv()
        take_z(7, 3, 7)

    def arrived(r):
        @pl.when(has_lo)
        def _():
            x_up(r).wait_recv()

        @pl.when(has_hi)
        def _():
            x_dn(r).wait_recv()

    arrived(0)
    arrived(nr - 1)

    for ok, k in ((y_hi, 0), (y_lo, 1)):
        @pl.when(ok)
        def _(k=k):
            y_edge[k].start()

        @pl.when(jnp.logical_and(ok, has_lo))
        def _(k=k):
            y_far[0][k].start()

        @pl.when(jnp.logical_and(ok, has_hi))
        def _(k=k):
            y_far[1][k].start()

    pass_on(2)
    lane = lax.broadcasted_iota(jnp.int32, (8, LANES), 1)

    def columns(tile):
        at = pl.ds(pl.multiple_of(tile * 8, 8), 8)
        sums = []
        for t in range(nt + 1):
            e = [ext[p, t, at, :] for p in range(10)]
            mid = (e[3] + e[4]) + (e[5] + e[6])
            lo2, hi2 = e[2] + e[1], e[7] + e[8]
            sums.append([mid + (lo2 + e[0]), mid + lo2 + e[7], mid + e[2] + hi2, mid + (hi2 + e[9])])
        for x in range(4):
            h = [sums[t][x] for t in range(nt + 1)]
            after = shifted(nt, roll_all(h, 1), 1, lane)
            before = shifted(nt, roll_all(h, -1), -1, lane)
            for t in range(nt):
                c0[x, t, at, :] = h[t]
                d0[x, t, at, :] = after[t] - before[t]
                s0[x, t, at, :] = after[t] + before[t] - 2.0 * h[t]
        for p in range(6):
            f = [ext[2 + p, t, at, :] for t in range(nt + 1)]
            pair = [a + b for a, b in zip(f, shifted(nt + 1, roll_all(f, 1), 1, lane))]
            quad = [a + b for a, b in zip(pair, shifted(nt + 1, roll_all(pair, 2), 2, lane))]
            back = shifted(nt, roll_all(quad, -3), -3, lane)
            for t in range(nt):
                c2[p, t, at, :] = back[t] + (quad[t] - f[t])

    def curve(tile):
        row = tile * 8
        own = pl.ds(pl.multiple_of(row - 8, 8), 8)
        at = pl.ds(pl.multiple_of(row, 8), 8)
        up, dn = pl.ds(row + 1, 8), pl.ds(row - 1, 8)
        col = []
        for p in range(6):
            parts = []
            for t in range(nt + 1):
                v = [ext[2 + p, t, pl.ds(row + k, 8), :] for k in range(-3, 4)]
                parts.append(((v[0] + v[1]) + (v[2] + v[3])) + ((v[4] + v[5]) + v[6]))
            after = shifted(nt, roll_all(parts, 1), 1, lane)
            before = shifted(nt, roll_all(parts, -1), -1, lane)
            col.append((parts, [a - b for a, b in zip(after, before)], [a + b for a, b in zip(after, before)]))
        best = vmax[...]
        for t in range(nt):
            across = pl.ds(t * LANES, LANES)
            for x in range(4):
                o = ori[x, own, across]
                is0, is1 = o == 0, o == 1

                def pick(a, b, c):
                    return jnp.where(is0, a, jnp.where(is1, b, c))

                h0 = c0[x, t, at, :]
                u0, w0 = c0[x, t, up, :], c0[x, t, dn, :]
                h1 = col[x + 1][0][t]
                u1, w1 = col[x + 2][0][t], col[x][0][t]
                h2 = c2[x + 1, t, at, :]
                u2, w2 = c2[x + 2, t, at, :], c2[x, t, at, :]
                b2u, b2w = c2[x + 1, t, up, :], c2[x + 1, t, dn, :]
                twist2 = (c2[x + 2, t, up, :] - c2[x + 2, t, dn, :]) - (c2[x, t, up, :] - c2[x, t, dn, :])
                centre = pick(h0, h1, h2)
                plus, minus = pick(u0, u1, u2), pick(w0, w1, w2)
                slope_a = 0.5 * (plus - minus)
                bend_a = plus + minus - 2.0 * centre
                slope_b = 0.5 * pick(d0[x, t, at, :], col[x + 1][1][t], b2u - b2w)
                bend_b = pick(s0[x, t, at, :], col[x + 1][2][t] - 2.0 * h1, b2u + b2w - 2.0 * h2)
                twist = pick(d0[x, t, up, :] - d0[x, t, dn, :], col[x + 2][1][t] - col[x][1][t], twist2)
                qa, qb = slope_a * slope_a, slope_b * slope_b
                numer = bend_a * (1.0 + qb) + bend_b * (1.0 + qa) - 0.5 * twist * (slope_a * slope_b)
                inv = lax.rsqrt(1.0 + qa + qb)
                kappa = jnp.where(itf[x, own, across] == 1, numer * (inv * inv * inv), 0.0)
                res[x, own, across] = kappa
                best = jnp.maximum(best, jnp.abs(kappa))
        vmax[...] = best

    for ok, k in ((y_lo, 0), (y_hi, 1)):
        @pl.when(ok)
        def _(k=k):
            y_own[k].wait_recv()
            y_edge[k].wait_recv()

        @pl.when(jnp.logical_and(ok, has_lo))
        def _(k=k):
            y_far[0][k].wait_recv()

        @pl.when(jnp.logical_and(ok, has_hi))
        def _(k=k):
            y_far[1][k].wait_recv()

    pass_on(3)
    load_ori.wait()
    load_itf.wait()

    def edges(i, carry):
        columns(i + jnp.where(i >= 2, nr - 2, 0))
        return carry

    lax.fori_loop(0, 4, edges, 0)
    pass_on(4)

    def middle(tile, carry):
        arrived(tile - 1)
        columns(tile)
        curve(tile - 1)
        return carry

    lax.fori_loop(2, nr, middle, 0)

    def tail(tile, carry):
        curve(tile)
        return carry

    lax.fori_loop(nr - 1, nr + 1, tail, 0)

    r1[me1] = jnp.max(vmax[...], axis=0, keepdims=True)

    def red1(k, sign=1):
        y, at = peer1(steps1[k], sign)
        slot = me1 if sign > 0 else y * ngy + at
        return remote(r1.at[slot], r1.at[slot], r1s.at[k], r1r.at[k], (y * zhi + z_at, at, gz))

    def red2(k, sign=1):
        i = peer2(steps2[k], sign)
        slot = me2 if sign > 0 else i
        return remote(r2.at[slot], r2.at[slot], r2s.at[k], r2r.at[k], (y_at * zhi + i // ngz, gy, lax.rem(i, ngz)))

    for d in range(n1 - 1):
        red1(d).start()
    for d in range(n1 - 1):
        red1(d, -1).wait_recv()
    r2[me2] = jnp.max(r1[...], axis=0)
    for d in range(n2 - 1):
        red2(d).start()

    z_own.wait_send()

    def sent_row(r, carry):
        @pl.when(has_hi)
        def _():
            x_up(r).wait_send()

        @pl.when(has_lo)
        def _():
            x_dn(r).wait_send()

        return carry

    lax.fori_loop(0, nr, sent_row, 0)

    @pl.when(has_hi)
    def _():
        z_up[0].wait_send()
        z_up[1].wait_send()

    @pl.when(has_lo)
    def _():
        z_dn[0].wait_send()
        z_dn[1].wait_send()

    for ok, k in ((y_hi, 0), (y_lo, 1)):
        @pl.when(ok)
        def _(k=k):
            y_own[k].wait_send()
            y_edge[k].wait_send()

        @pl.when(jnp.logical_and(ok, has_lo))
        def _(k=k):
            y_far[0][k].wait_send()

        @pl.when(jnp.logical_and(ok, has_hi))
        def _(k=k):
            y_far[1][k].wait_send()

    for d in range(n1 - 1):
        red1(d).wait_send()
    for d in range(n2 - 1):
        red2(d, -1).wait_recv()
    peak_ref[...] = jnp.max(r2[...], axis=0)
    for d in range(n2 - 1):
        red2(d).wait_send()


def settle(res, peak, out, peak_out, top, sems):
    copies = [pltpu.make_async_copy(res.at[p], out.at[p], sems.at[p]) for p in range(res.shape[0])]
    for copy in copies:
        copy.start()
    top[0, 0] = jnp.max(peak[...])
    last = pltpu.make_async_copy(top, peak_out, sems.at[res.shape[0]])
    last.start()
    last.wait()
    for copy in copies:
        copy.wait()


def block(sizes, fraction, orientation, interface):
    planes, rows, lanes = fraction.shape
    ngx, ngy, ngz, zhi = sizes
    nt, nr = lanes // LANES, rows // 8
    n1, n2 = (ngx // zhi) * ngy, zhi * ngz
    hops = ngy // 4 + ngx // zhi // 2 + 1
    dma = pltpu.SemaphoreType.DMA
    f32 = jnp.float32
    curvature, peak = pl.pallas_call(
        functools.partial(kernel, sizes),
        out_shape=(
            jax.ShapeDtypeStruct(fraction.shape, f32),
            jax.ShapeDtypeStruct((1, LANES), f32),
        ),
        in_specs=[pl.BlockSpec(memory_space=pl.ANY)] * 3,
        out_specs=(pl.BlockSpec(memory_space=pltpu.VMEM), pl.BlockSpec(memory_space=pltpu.VMEM)),
        scratch_shapes=[
            pltpu.VMEM((10, nt + 1, rows + 16, LANES), f32),
            pltpu.VMEM((4, nt, rows + 16, LANES), f32),
            pltpu.VMEM((4, nt, rows + 16, LANES), f32),
            pltpu.VMEM((4, nt, rows + 16, LANES), f32),
            pltpu.VMEM((6, nt, rows + 16, LANES), f32),
            pltpu.VMEM((planes, rows, lanes), jnp.int32),
            pltpu.VMEM((planes, rows, lanes), jnp.int32),
            pltpu.VMEM((4, 3, 1, LANES), f32),
            pltpu.VMEM((10, 3, 1, LANES), f32),
            pltpu.VMEM((10, 8, LANES), f32),
            pltpu.VMEM((8, LANES), f32),
            pltpu.VMEM((n1, 1, LANES), f32),
            pltpu.VMEM((n2, 1, LANES), f32),
            dma((nt + 2,)),
            dma((2, nr)), dma((2, nr)),
            dma((2,)), dma((2,)),
            dma((2,)), dma((2,)),
            dma((2, 2)), dma((2, 2)),
            dma((5,)), dma((5,)),
            dma((n1,)), dma((n1,)),
            dma((n2,)), dma((n2,)),
            pltpu.SemaphoreType.REGULAR((hops - 1,)),
        ],
        compiler_params=pltpu.CompilerParams(
            collective_id=0, has_side_effects=True, vmem_limit_bytes=55000000
        ),
    )(fraction, orientation, interface)
    curvature, peak = pl.pallas_call(
        settle,
        out_shape=(
            jax.ShapeDtypeStruct(fraction.shape, f32),
            jax.ShapeDtypeStruct((1, 1), f32),
        ),
        in_specs=[pl.BlockSpec(memory_space=pltpu.VMEM), pl.BlockSpec(memory_space=pltpu.VMEM)],
        out_specs=(pl.BlockSpec(memory_space=pl.ANY),) * 2,
        scratch_shapes=[pltpu.SMEM((1, 1), f32), dma((planes + 1,))], compiler_params=pltpu.CompilerParams(vmem_limit_bytes=1048576 * 2),
    )(curvature, peak)
    return curvature, peak.reshape(())


def solution(mesh):
    sizes = (mesh.shape["gx"], mesh.shape["gy"], mesh.shape["gz"], min(Z_HI, mesh.shape["gx"]))
    spec = P("gx", "gy", "gz")
    return jax.shard_map(
        functools.partial(block, sizes), mesh=mesh, in_specs=(spec,) * 3, out_specs=(spec, P()), check_vma=False
    )
```

```python
import functools

import jax
import jax.numpy as jnp
from jax import lax
from jax.experimental import pallas as pl
from jax.experimental.pallas import tpu as pltpu
from jax.sharding import PartitionSpec as P

MESH = pl.DeviceIdType.MESH
LANES = 128
Z_HI = 4


def shifted(tiles, rolled, shift, lane):
    count = len(rolled)
    out = []
    for t in range(tiles):
        if shift > 0:
            out.append(jnp.where(lane >= LANES - shift, rolled[(t + 1) % count], rolled[t]))
        else:
            out.append(jnp.where(lane < -shift, rolled[(t - 1) % count], rolled[t]))
    return out


def roll_all(tiles, shift):
    return [pltpu.roll(x, (-shift) % LANES, x.ndim - 1) for x in tiles]


def kernel(
    sizes, f_hbm, ori_hbm, itf_hbm, res, peak_ref,
    ext, c0, d0, s0, c2, ori, itf, zs, zr, zt, vmax, r1, r2,
    load_sem, xs, xr, ys, yr, y4s, y4r, yxs, yxr, zss, zrs, r1s, r1r, r2s, r2r, tok,
):
    ngx, ngy, ngz, zhi = sizes
    gx, gy, gz = lax.axis_index("gx"), lax.axis_index("gy"), lax.axis_index("gz")
    other = 1 - gz
    planes, rows, lanes = f_hbm.shape
    nt = lanes // LANES
    nr = rows // 8
    has_lo, has_hi = gx > 0, gx < ngx - 1
    y_lo, y_hi = gy > 0, gy < ngy - 1
    top = 8 + rows

    loads = [
        pltpu.make_async_copy(
            f_hbm.at[:, :, pl.ds(t * LANES, LANES)], ext.at[pl.ds(3, 4), t, pl.ds(8, rows), :],
            load_sem.at[t])
        for t in range(nt)
    ]
    load_ori = pltpu.make_async_copy(ori_hbm, ori, load_sem.at[nt])
    load_itf = pltpu.make_async_copy(itf_hbm, itf, load_sem.at[nt + 1])
    ny, nx = ngx // zhi, ngy // 2
    y_at, z_at = gx // zhi, gx % zhi
    x_at, core = gy // 2, lax.rem(gy, 2)
    n1, n2 = ny * ngy, zhi * ngz
    me1, me2 = y_at * ngy + gy, z_at * ngz + gz

    def around(d, n):
        return min(d, n - d)

    steps1 = [(dy, dx, dc) for dy in range(ny) for dx in range(nx) for dc in range(2)][1:]
    steps1.sort(key=lambda d: (-around(d[0], ny) - around(d[1], nx), -d[2]))
    steps2 = sorted(range(1, n2), key=lambda d: -around(d, n2))

    def peer1(step, sign):
        dy, dx, dc = step
        y = lax.rem(y_at + sign * dy + ny, ny)
        x = lax.rem(x_at + sign * dx + nx, nx)
        return y, x * 2 + (1 - core if dc else core)

    def peer2(d, sign):
        return lax.rem(me2 + sign * d + n2, n2)

    def steps(n):
        return (1, n - 1) if n > 2 else (1,) * (n - 1)

    ring = [(y_at * zhi + lax.rem(z_at + d, zhi), gy, gz) for d in steps(zhi)]
    ring += [(lax.rem(y_at + d, ny) * zhi + z_at, gy, gz) for d in steps(ny)]
    ring += [(gx, lax.rem(x_at + d, nx) * 2 + core, gz) for d in steps(nx)]
    ring += [(gx, gy, other), (gx, gy + 1 - 2 * core, gz)]
    barrier = pltpu.get_barrier_semaphore()

    def tell(semaphore, device):
        pl.semaphore_signal(semaphore, inc=1, device_id=device, device_id_type=MESH)

    extra = (
        (jnp.logical_and(has_hi, z_at == zhi - 1), (gx + 1, gy, gz)),
        (jnp.logical_and(has_lo, z_at == 0), (gx - 1, gy, gz)),
        (jnp.logical_and(y_hi, core == 1), (gx, gy + 1, gz)),
        (jnp.logical_and(y_lo, core == 0), (gx, gy - 1, gz)),
    )
    for ok, device in extra:
        @pl.when(ok)
        def _(device=device):
            tell(barrier, device)

    for device in ring:
        tell(barrier, device)
    for copy in loads:
        copy.start()
    load_ori.start()
    load_itf.start()
    greeted = len(ring)
    for ok, _ in extra:
        greeted = greeted + jnp.where(ok, 1, 0)

    @pl.when(jnp.logical_not(has_lo))
    def _():
        ext[0:3] = jnp.zeros((3, nt + 1, rows + 16, LANES), jnp.float32)

    @pl.when(jnp.logical_not(has_hi))
    def _():
        ext[7:10] = jnp.zeros((3, nt + 1, rows + 16, LANES), jnp.float32)

    @pl.when(jnp.logical_not(y_lo))
    def _():
        ext[:, :, 0:8] = jnp.zeros((10, nt + 1, 8, LANES), jnp.float32)

    @pl.when(jnp.logical_not(y_hi))
    def _():
        ext[:, :, top:top + 8] = jnp.zeros((10, nt + 1, 8, LANES), jnp.float32)

    for copy in loads:
        copy.wait()

    edge = jnp.where(gz == 0, nt - 1, 0)
    for p in range(4):
        turned = jnp.transpose(ext[3 + p, edge, 8:top, :])
        part = jnp.where(gz == 0, turned[LANES - 3:LANES], turned[0:3])
        for c in range(3):
            zs[p, c] = part[c:c + 1]
    zt[...] = jnp.zeros_like(zt)
    vmax[...] = jnp.zeros_like(vmax)

    pl.semaphore_wait(barrier, greeted)

    def remote(src, dst, send, recv, device):
        return pltpu.make_async_remote_copy(
            src_ref=src, dst_ref=dst, send_sem=send, recv_sem=recv, device_id=device,
            device_id_type=MESH)

    nearest = 2 * gz
    z_own = remote(zs, zr.at[pl.ds(3, 4)], zss.at[0], zrs.at[0], (gx, gy, other))
    z_up = (
        remote(zr.at[6], zr.at[2], zss.at[1], zrs.at[1], (gx + 1, gy, gz)),
        remote(zr.at[pl.ds(4, 2), nearest], zr.at[pl.ds(0, 2), nearest], zss.at[2], zrs.at[2], (gx + 1, gy, gz)),
    )
    z_dn = (
        remote(zr.at[3], zr.at[7], zss.at[3], zrs.at[3], (gx - 1, gy, gz)),
        remote(zr.at[pl.ds(4, 2), nearest], zr.at[pl.ds(8, 2), nearest], zss.at[4], zrs.at[4], (gx - 1, gy, gz)),
    )

    def x_up(r):
        at = pl.ds(pl.multiple_of(8 + r * 8, 8), 8)
        return remote(ext.at[pl.ds(4, 3), pl.ds(0, nt), at, :], ext.at[pl.ds(0, 3), pl.ds(0, nt), at, :],
                      xs.at[0, r], xr.at[0, r], (gx + 1, gy, gz))

    def x_dn(r):
        at = pl.ds(pl.multiple_of(8 + r * 8, 8), 8)
        return remote(ext.at[pl.ds(3, 3), pl.ds(0, nt), at, :], ext.at[pl.ds(7, 3), pl.ds(0, nt), at, :],
                      xs.at[1, r], xr.at[1, r], (gx - 1, gy, gz))

    def y_up(first, count, t0, tn, send, recv):
        return remote(ext.at[pl.ds(first, count), pl.ds(t0, tn), pl.ds(rows, 8), :],
                      ext.at[pl.ds(first, count), pl.ds(t0, tn), pl.ds(0, 8), :], send, recv,
                      (gx, gy + 1, gz))

    def y_dn(first, count, t0, tn, send, recv):
        return remote(ext.at[pl.ds(first, count), pl.ds(t0, tn), pl.ds(8, 8), :],
                      ext.at[pl.ds(first, count), pl.ds(t0, tn), pl.ds(top, 8), :], send, recv,
                      (gx, gy - 1, gz))

    y_own = (y_up(3, 4, 0, nt, ys.at[0], yr.at[0]), y_dn(3, 4, 0, nt, ys.at[1], yr.at[1]))
    y_edge = (y_up(3, 4, nt, 1, y4s.at[0], y4r.at[0]), y_dn(3, 4, nt, 1, y4s.at[1], y4r.at[1]))
    y_far = [
        (y_up(first, 3, 0, nt + 1, yxs.at[0, s], yxr.at[0, s]), y_dn(first, 3, 0, nt + 1, yxs.at[1, s], yxr.at[1, s]))
        for s, first in ((0, 0), (1, 7))
    ]

    z_own.start()

    @pl.when(has_hi)
    def _():
        x_up(0).start()
        x_up(nr - 1).start()

    @pl.when(has_lo)
    def _():
        x_dn(0).start()
        x_dn(nr - 1).start()

    @pl.when(y_hi)
    def _():
        y_own[0].start()

    @pl.when(y_lo)
    def _():
        y_own[1].start()

    def send_row(r, carry):
        @pl.when(has_hi)
        def _():
            x_up(r).start()

        @pl.when(has_lo)
        def _():
            x_dn(r).start()

        return carry

    first_rows = 1
    lax.fori_loop(1, first_rows, send_row, 0)
    def pass_on(level):
        if level > 0 and level <= tok.shape[0]:
            pl.semaphore_wait(tok.at[level - 1], len(ring))
        if level < tok.shape[0]:
            for device in ring:
                tell(tok.at[level], device)

    pass_on(0)

    def take_z(first, count, near):
        for p in range(first, first + count):
            if near is None or p == near:
                for c in range(3):
                    zt[p, pl.ds(5 * gz + c, 1), :] = zr[p, c]
            else:
                zt[p, pl.ds(5 * gz + nearest, 1), :] = zr[p, nearest]
        for p in range(first, first + count):
            part = zt[p]
            zero = jnp.zeros_like(part)
            low, high = jnp.where(gz == 0, part, zero), jnp.where(gz == 0, zero, part)
            between = jnp.zeros((LANES - 16, LANES), jnp.float32)
            ext[p, nt, 8:top, :] = jnp.transpose(jnp.concatenate([low, between, high], axis=0))

    z_own.wait_recv()

    @pl.when(has_hi)
    def _():
        z_up[0].start()
        z_up[1].start()

    @pl.when(has_lo)
    def _():
        z_dn[0].start()
        z_dn[1].start()

    lax.fori_loop(first_rows, nr - 1, send_row, 0)
    take_z(3, 4, None)
    pass_on(1)

    @pl.when(has_lo)
    def _():
        z_up[0].wait_recv()
        z_up[1].wait_recv()
        take_z(0, 3, 2)

    @pl.when(has_hi)
    def _():
        z_dn[0].wait_recv()
        z_dn[1].wait_recv()
        take_z(7, 3, 7)

    def arrived(r):
        @pl.when(has_lo)
        def _():
            x_up(r).wait_recv()

        @pl.when(has_hi)
        def _():
            x_dn(r).wait_recv()

    arrived(0)
    arrived(nr - 1)

    for ok, k in ((y_hi, 0), (y_lo, 1)):
        @pl.when(ok)
        def _(k=k):
            y_edge[k].start()

        @pl.when(jnp.logical_and(ok, has_lo))
        def _(k=k):
            y_far[0][k].start()

        @pl.when(jnp.logical_and(ok, has_hi))
        def _(k=k):
            y_far[1][k].start()

    pass_on(2)
    lane = lax.broadcasted_iota(jnp.int32, (8, LANES), 1)

    def columns(tile):
        at = pl.ds(pl.multiple_of(tile * 8, 8), 8)
        sums = []
        for t in range(nt + 1):
            e = [ext[p, t, at, :] for p in range(10)]
            mid = (e[3] + e[4]) + (e[5] + e[6])
            lo2, hi2 = e[2] + e[1], e[7] + e[8]
            sums.append([mid + (lo2 + e[0]), mid + lo2 + e[7], mid + e[2] + hi2, mid + (hi2 + e[9])])
        for x in range(4):
            h = [sums[t][x] for t in range(nt + 1)]
            after = shifted(nt, roll_all(h, 1), 1, lane)
            before = shifted(nt, roll_all(h, -1), -1, lane)
            for t in range(nt):
                c0[x, t, at, :] = h[t]
                d0[x, t, at, :] = after[t] - before[t]
                s0[x, t, at, :] = after[t] + before[t] - 2.0 * h[t]
        for p in range(6):
            f = [ext[2 + p, t, at, :] for t in range(nt + 1)]
            pair = [a + b for a, b in zip(f, shifted(nt + 1, roll_all(f, 1), 1, lane))]
            quad = [a + b for a, b in zip(pair, shifted(nt + 1, roll_all(pair, 2), 2, lane))]
            back = shifted(nt, roll_all(quad, -3), -3, lane)
            for t in range(nt):
                c2[p, t, at, :] = back[t] + (quad[t] - f[t])

    def curve(tile):
        row = tile * 8
        own = pl.ds(pl.multiple_of(row - 8, 8), 8)
        at = pl.ds(pl.multiple_of(row, 8), 8)
        up, dn = pl.ds(row + 1, 8), pl.ds(row - 1, 8)
        col = []
        for p in range(6):
            parts = []
            for t in range(nt + 1):
                v = [ext[2 + p, t, pl.ds(row + k, 8), :] for k in range(-3, 4)]
                parts.append(((v[0] + v[1]) + (v[2] + v[3])) + ((v[4] + v[5]) + v[6]))
            after = shifted(nt, roll_all(parts, 1), 1, lane)
            before = shifted(nt, roll_all(parts, -1), -1, lane)
            col.append((parts, [a - b for a, b in zip(after, before)], [a + b for a, b in zip(after, before)]))
        best = vmax[...]
        for t in range(nt):
            across = pl.ds(t * LANES, LANES)
            for x in range(4):
                o = ori[x, own, across]
                is0, is1 = o == 0, o == 1

                def pick(a, b, c):
                    return jnp.where(is0, a, jnp.where(is1, b, c))

                h0 = c0[x, t, at, :]
                u0, w0 = c0[x, t, up, :], c0[x, t, dn, :]
                h1 = col[x + 1][0][t]
                u1, w1 = col[x + 2][0][t], col[x][0][t]
                h2 = c2[x + 1, t, at, :]
                u2, w2 = c2[x + 2, t, at, :], c2[x, t, at, :]
                b2u, b2w = c2[x + 1, t, up, :], c2[x + 1, t, dn, :]
                twist2 = (c2[x + 2, t, up, :] - c2[x + 2, t, dn, :]) - (c2[x, t, up, :] - c2[x, t, dn, :])
                centre = pick(h0, h1, h2)
                plus, minus = pick(u0, u1, u2), pick(w0, w1, w2)
                slope_a = 0.5 * (plus - minus)
                bend_a = plus + minus - 2.0 * centre
                slope_b = 0.5 * pick(d0[x, t, at, :], col[x + 1][1][t], b2u - b2w)
                bend_b = pick(s0[x, t, at, :], col[x + 1][2][t] - 2.0 * h1, b2u + b2w - 2.0 * h2)
                twist = pick(d0[x, t, up, :] - d0[x, t, dn, :], col[x + 2][1][t] - col[x][1][t], twist2)
                qa, qb = slope_a * slope_a, slope_b * slope_b
                numer = bend_a * (1.0 + qb) + bend_b * (1.0 + qa) - 0.5 * twist * (slope_a * slope_b)
                inv = lax.rsqrt(1.0 + qa + qb)
                kappa = jnp.where(itf[x, own, across] == 1, numer * (inv * inv * inv), 0.0)
                res[x, own, across] = kappa
                best = jnp.maximum(best, jnp.abs(kappa))
        vmax[...] = best

    for ok, k in ((y_lo, 0), (y_hi, 1)):
        @pl.when(ok)
        def _(k=k):
            y_own[k].wait_recv()
            y_edge[k].wait_recv()

        @pl.when(jnp.logical_and(ok, has_lo))
        def _(k=k):
            y_far[0][k].wait_recv()

        @pl.when(jnp.logical_and(ok, has_hi))
        def _(k=k):
            y_far[1][k].wait_recv()

    pass_on(3)
    load_ori.wait()
    load_itf.wait()

    def edges(i, carry):
        columns(i + jnp.where(i >= 2, nr - 2, 0))
        return carry

    lax.fori_loop(0, 4, edges, 0)
    pass_on(4)

    def middle(tile, carry):
        arrived(tile - 1)
        columns(tile)
        curve(tile - 1)
        return carry

    lax.fori_loop(2, nr, middle, 0)

    def tail(tile, carry):
        curve(tile)
        return carry

    lax.fori_loop(nr - 1, nr + 1, tail, 0)

    r1[me1] = jnp.max(vmax[...], axis=0, keepdims=True)

    def red1(k, sign=1):
        y, at = peer1(steps1[k], sign)
        slot = me1 if sign > 0 else y * ngy + at
        return remote(r1.at[slot], r1.at[slot], r1s.at[k], r1r.at[k], (y * zhi + z_at, at, gz))

    def red2(k, sign=1):
        i = peer2(steps2[k], sign)
        slot = me2 if sign > 0 else i
        return remote(r2.at[slot], r2.at[slot], r2s.at[k], r2r.at[k], (y_at * zhi + i // ngz, gy, lax.rem(i, ngz)))

    for d in range(n1 - 1):
        red1(d).start()
    for d in range(n1 - 1):
        red1(n1 - 2 - d, -1).wait_recv()
    r2[me2] = jnp.max(r1[...], axis=0)
    for d in range(n2 - 1):
        red2(d).start()

    z_own.wait_send()

    def sent_row(r, carry):
        @pl.when(has_hi)
        def _():
            x_up(r).wait_send()

        @pl.when(has_lo)
        def _():
            x_dn(r).wait_send()

        return carry

    lax.fori_loop(0, nr, sent_row, 0)

    @pl.when(has_hi)
    def _():
        z_up[0].wait_send()
        z_up[1].wait_send()

    @pl.when(has_lo)
    def _():
        z_dn[0].wait_send()
        z_dn[1].wait_send()

    for ok, k in ((y_hi, 0), (y_lo, 1)):
        @pl.when(ok)
        def _(k=k):
            y_own[k].wait_send()
            y_edge[k].wait_send()

        @pl.when(jnp.logical_and(ok, has_lo))
        def _(k=k):
            y_far[0][k].wait_send()

        @pl.when(jnp.logical_and(ok, has_hi))
        def _(k=k):
            y_far[1][k].wait_send()

    for d in range(n1 - 1):
        red1(d).wait_send()
    for d in range(n2 - 1):
        red2(n2 - 2 - d, -1).wait_recv()
    peak_ref[...] = jnp.max(r2[...], axis=0)
    for d in range(n2 - 1):
        red2(d).wait_send()


def settle(res, peak, out, peak_out, top, sems):
    copies = [pltpu.make_async_copy(res.at[p], out.at[p], sems.at[p]) for p in range(res.shape[0])]
    for copy in copies:
        copy.start()
    top[0, 0] = jnp.max(peak[...])
    last = pltpu.make_async_copy(top, peak_out, sems.at[res.shape[0]])
    last.start()
    last.wait()
    for copy in copies:
        copy.wait()


def block(sizes, fraction, orientation, interface):
    planes, rows, lanes = fraction.shape
    ngx, ngy, ngz, zhi = sizes
    nt, nr = lanes // LANES, rows // 8
    n1, n2 = (ngx // zhi) * ngy, zhi * ngz
    hops = ngy // 4 + ngx // zhi // 2 + 1
    dma = pltpu.SemaphoreType.DMA
    f32 = jnp.float32
    curvature, peak = pl.pallas_call(
        functools.partial(kernel, sizes),
        out_shape=(
            jax.ShapeDtypeStruct(fraction.shape, f32),
            jax.ShapeDtypeStruct((1, LANES), f32),
        ),
        in_specs=[pl.BlockSpec(memory_space=pl.ANY)] * 3,
        out_specs=(pl.BlockSpec(memory_space=pltpu.VMEM), pl.BlockSpec(memory_space=pltpu.VMEM)),
        scratch_shapes=[
            pltpu.VMEM((10, nt + 1, rows + 16, LANES), f32),
            pltpu.VMEM((4, nt, rows + 16, LANES), f32),
            pltpu.VMEM((4, nt, rows + 16, LANES), f32),
            pltpu.VMEM((4, nt, rows + 16, LANES), f32),
            pltpu.VMEM((6, nt, rows + 16, LANES), f32),
            pltpu.VMEM((planes, rows, lanes), jnp.int32),
            pltpu.VMEM((planes, rows, lanes), jnp.int32),
            pltpu.VMEM((4, 3, 1, LANES), f32),
            pltpu.VMEM((10, 3, 1, LANES), f32),
            pltpu.VMEM((10, 8, LANES), f32),
            pltpu.VMEM((8, LANES), f32),
            pltpu.VMEM((n1, 1, LANES), f32),
            pltpu.VMEM((n2, 1, LANES), f32),
            dma((nt + 2,)),
            dma((2, nr)), dma((2, nr)),
            dma((2,)), dma((2,)),
            dma((2,)), dma((2,)),
            dma((2, 2)), dma((2, 2)),
            dma((5,)), dma((5,)),
            dma((n1,)), dma((n1,)),
            dma((n2,)), dma((n2,)),
            pltpu.SemaphoreType.REGULAR((hops - 1,)),
        ],
        compiler_params=pltpu.CompilerParams(
            collective_id=0, has_side_effects=True, vmem_limit_bytes=55000000
        ),
    )(fraction, orientation, interface)
    curvature, peak = pl.pallas_call(
        settle,
        out_shape=(
            jax.ShapeDtypeStruct(fraction.shape, f32),
            jax.ShapeDtypeStruct((1, 1), f32),
        ),
        in_specs=[pl.BlockSpec(memory_space=pltpu.VMEM), pl.BlockSpec(memory_space=pltpu.VMEM)],
        out_specs=(pl.BlockSpec(memory_space=pl.ANY),) * 2,
        scratch_shapes=[pltpu.SMEM((1, 1), f32), dma((planes + 1,))], compiler_params=pltpu.CompilerParams(vmem_limit_bytes=1048576 * 2),
    )(curvature, peak)
    return curvature, peak.reshape(())


def solution(mesh):
    sizes = (mesh.shape["gx"], mesh.shape["gy"], mesh.shape["gz"], min(Z_HI, mesh.shape["gx"]))
    spec = P("gx", "gy", "gz")
    return jax.shard_map(
        functools.partial(block, sizes), mesh=mesh, in_specs=(spec,) * 3, out_specs=(spec, P()), check_vma=False
    )
```

```python
import functools

import jax
import jax.numpy as jnp
from jax import lax
from jax.experimental import pallas as pl
from jax.experimental.pallas import tpu as pltpu
from jax.sharding import PartitionSpec as P

MESH = pl.DeviceIdType.MESH
LANES = 128
Z_HI = 4


def shifted(tiles, rolled, shift, lane):
    count = len(rolled)
    out = []
    for t in range(tiles):
        if shift > 0:
            out.append(jnp.where(lane >= LANES - shift, rolled[(t + 1) % count], rolled[t]))
        else:
            out.append(jnp.where(lane < -shift, rolled[(t - 1) % count], rolled[t]))
    return out


def roll_all(tiles, shift):
    return [pltpu.roll(x, (-shift) % LANES, x.ndim - 1) for x in tiles]


def kernel(
    sizes, f_hbm, ori_hbm, itf_hbm, res, peak_ref,
    ext, c0, d0, s0, c2, ori, itf, zs, zr, zt, vmax, r1, r2,
    load_sem, xs, xr, ys, yr, y4s, y4r, yxs, yxr, zss, zrs, r1s, r1r, r2s, r2r, tok,
):
    ngx, ngy, ngz, zhi = sizes
    gx, gy, gz = lax.axis_index("gx"), lax.axis_index("gy"), lax.axis_index("gz")
    other = 1 - gz
    planes, rows, lanes = f_hbm.shape
    nt = lanes // LANES
    nr = rows // 8
    has_lo, has_hi = gx > 0, gx < ngx - 1
    y_lo, y_hi = gy > 0, gy < ngy - 1
    top = 8 + rows

    loads = [
        pltpu.make_async_copy(
            f_hbm.at[:, :, pl.ds(t * LANES, LANES)], ext.at[pl.ds(3, 4), t, pl.ds(8, rows), :],
            load_sem.at[t])
        for t in range(nt)
    ]
    load_ori = pltpu.make_async_copy(ori_hbm, ori, load_sem.at[nt])
    load_itf = pltpu.make_async_copy(itf_hbm, itf, load_sem.at[nt + 1])
    ny, nx = ngx // zhi, ngy // 2
    y_at, z_at = gx // zhi, gx % zhi
    x_at, core = gy // 2, lax.rem(gy, 2)
    n1, n2 = ny * ngy, zhi * ngz
    me1, me2 = y_at * ngy + gy, z_at * ngz + gz

    def around(d, n):
        return min(d, n - d)

    steps1 = [(dy, dx, dc) for dy in range(ny) for dx in range(nx) for dc in range(2)][1:]
    steps1.sort(key=lambda d: (-around(d[0], ny) - around(d[1], nx), -d[2]))
    steps2 = sorted(range(1, n2), key=lambda d: -around(d, n2))

    def peer1(step, sign):
        dy, dx, dc = step
        y = lax.rem(y_at + sign * dy + ny, ny)
        x = lax.rem(x_at + sign * dx + nx, nx)
        return y, x * 2 + (1 - core if dc else core)

    def peer2(d, sign):
        return lax.rem(me2 + sign * d + n2, n2)

    def steps(n):
        return (1, n - 1) if n > 2 else (1,) * (n - 1)

    ring = [(y_at * zhi + lax.rem(z_at + d, zhi), gy, gz) for d in steps(zhi)]
    ring += [(lax.rem(y_at + d, ny) * zhi + z_at, gy, gz) for d in steps(ny)]
    ring += [(gx, lax.rem(x_at + d, nx) * 2 + core, gz) for d in steps(nx)]
    ring += [(gx, gy, other), (gx, gy + 1 - 2 * core, gz)]
    barrier = pltpu.get_barrier_semaphore()

    def tell(semaphore, device):
        pl.semaphore_signal(semaphore, inc=1, device_id=device, device_id_type=MESH)

    extra = (
        (jnp.logical_and(has_hi, z_at == zhi - 1), (gx + 1, gy, gz)),
        (jnp.logical_and(has_lo, z_at == 0), (gx - 1, gy, gz)),
        (jnp.logical_and(y_hi, core == 1), (gx, gy + 1, gz)),
        (jnp.logical_and(y_lo, core == 0), (gx, gy - 1, gz)),
    )
    for ok, device in extra:
        @pl.when(ok)
        def _(device=device):
            tell(barrier, device)

    for device in ring:
        tell(barrier, device)
    for copy in loads:
        copy.start()
    load_ori.start()
    load_itf.start()
    greeted = len(ring)
    for ok, _ in extra:
        greeted = greeted + jnp.where(ok, 1, 0)

    @pl.when(jnp.logical_not(has_lo))
    def _():
        ext[0:3] = jnp.zeros((3, nt + 1, rows + 16, LANES), jnp.float32)

    @pl.when(jnp.logical_not(has_hi))
    def _():
        ext[7:10] = jnp.zeros((3, nt + 1, rows + 16, LANES), jnp.float32)

    @pl.when(jnp.logical_not(y_lo))
    def _():
        ext[:, :, 0:8] = jnp.zeros((10, nt + 1, 8, LANES), jnp.float32)

    @pl.when(jnp.logical_not(y_hi))
    def _():
        ext[:, :, top:top + 8] = jnp.zeros((10, nt + 1, 8, LANES), jnp.float32)

    for copy in loads:
        copy.wait()

    edge = jnp.where(gz == 0, nt - 1, 0)
    for p in range(4):
        turned = jnp.transpose(ext[3 + p, edge, 8:top, :])
        part = jnp.where(gz == 0, turned[LANES - 3:LANES], turned[0:3])
        for c in range(3):
            zs[p, c] = part[c:c + 1]
    zt[...] = jnp.zeros_like(zt)
    vmax[...] = jnp.zeros_like(vmax)

    pl.semaphore_wait(barrier, greeted)

    def remote(src, dst, send, recv, device):
        return pltpu.make_async_remote_copy(
            src_ref=src, dst_ref=dst, send_sem=send, recv_sem=recv, device_id=device,
            device_id_type=MESH)

    nearest = 2 * gz
    z_own = remote(zs, zr.at[pl.ds(3, 4)], zss.at[0], zrs.at[0], (gx, gy, other))
    z_up = (
        remote(zr.at[6], zr.at[2], zss.at[1], zrs.at[1], (gx + 1, gy, gz)),
        remote(zr.at[pl.ds(4, 2), nearest], zr.at[pl.ds(0, 2), nearest], zss.at[2], zrs.at[2], (gx + 1, gy, gz)),
    )
    z_dn = (
        remote(zr.at[3], zr.at[7], zss.at[3], zrs.at[3], (gx - 1, gy, gz)),
        remote(zr.at[pl.ds(4, 2), nearest], zr.at[pl.ds(8, 2), nearest], zss.at[4], zrs.at[4], (gx - 1, gy, gz)),
    )

    def x_up(r):
        at = pl.ds(pl.multiple_of(8 + r * 8, 8), 8)
        return remote(ext.at[pl.ds(4, 3), pl.ds(0, nt), at, :], ext.at[pl.ds(0, 3), pl.ds(0, nt), at, :],
                      xs.at[0, r], xr.at[0, r], (gx + 1, gy, gz))

    def x_dn(r):
        at = pl.ds(pl.multiple_of(8 + r * 8, 8), 8)
        return remote(ext.at[pl.ds(3, 3), pl.ds(0, nt), at, :], ext.at[pl.ds(7, 3), pl.ds(0, nt), at, :],
                      xs.at[1, r], xr.at[1, r], (gx - 1, gy, gz))

    def y_up(first, count, t0, tn, send, recv):
        return remote(ext.at[pl.ds(first, count), pl.ds(t0, tn), pl.ds(rows, 8), :],
                      ext.at[pl.ds(first, count), pl.ds(t0, tn), pl.ds(0, 8), :], send, recv,
                      (gx, gy + 1, gz))

    def y_dn(first, count, t0, tn, send, recv):
        return remote(ext.at[pl.ds(first, count), pl.ds(t0, tn), pl.ds(8, 8), :],
                      ext.at[pl.ds(first, count), pl.ds(t0, tn), pl.ds(top, 8), :], send, recv,
                      (gx, gy - 1, gz))

    y_own = (y_up(3, 4, 0, nt, ys.at[0], yr.at[0]), y_dn(3, 4, 0, nt, ys.at[1], yr.at[1]))
    y_edge = (y_up(3, 4, nt, 1, y4s.at[0], y4r.at[0]), y_dn(3, 4, nt, 1, y4s.at[1], y4r.at[1]))
    y_far = [
        (y_up(first, 3, 0, nt + 1, yxs.at[0, s], yxr.at[0, s]), y_dn(first, 3, 0, nt + 1, yxs.at[1, s], yxr.at[1, s]))
        for s, first in ((0, 0), (1, 7))
    ]

    z_own.start()

    @pl.when(has_hi)
    def _():
        x_up(0).start()
        x_up(nr - 1).start()

    @pl.when(has_lo)
    def _():
        x_dn(0).start()
        x_dn(nr - 1).start()

    @pl.when(y_hi)
    def _():
        y_own[0].start()

    @pl.when(y_lo)
    def _():
        y_own[1].start()

    def send_row(r, carry):
        @pl.when(has_hi)
        def _():
            x_up(r).start()

        @pl.when(has_lo)
        def _():
            x_dn(r).start()

        return carry

    first_rows = 1
    lax.fori_loop(1, first_rows, send_row, 0)
    def pass_on(level):
        if level > 0 and level <= tok.shape[0]:
            pl.semaphore_wait(tok.at[level - 1], len(ring))
        if level < tok.shape[0]:
            for device in ring:
                tell(tok.at[level], device)

    pass_on(0)

    def take_z(first, count, near):
        for p in range(first, first + count):
            if near is None or p == near:
                for c in range(3):
                    zt[p, pl.ds(5 * gz + c, 1), :] = zr[p, c]
            else:
                zt[p, pl.ds(5 * gz + nearest, 1), :] = zr[p, nearest]
        for p in range(first, first + count):
            part = zt[p]
            zero = jnp.zeros_like(part)
            low, high = jnp.where(gz == 0, part, zero), jnp.where(gz == 0, zero, part)
            between = jnp.zeros((LANES - 16, LANES), jnp.float32)
            ext[p, nt, 8:top, :] = jnp.transpose(jnp.concatenate([low, between, high], axis=0))

    z_own.wait_recv()

    @pl.when(has_hi)
    def _():
        z_up[0].start()
        z_up[1].start()

    @pl.when(has_lo)
    def _():
        z_dn[0].start()
        z_dn[1].start()

    lax.fori_loop(first_rows, nr - 1, send_row, 0)
    take_z(3, 4, None)
    pass_on(1)

    @pl.when(has_lo)
    def _():
        z_up[0].wait_recv()
        z_up[1].wait_recv()
        take_z(0, 3, 2)

    @pl.when(has_hi)
    def _():
        z_dn[0].wait_recv()
        z_dn[1].wait_recv()
        take_z(7, 3, 7)

    def arrived(r):
        @pl.when(has_lo)
        def _():
            x_up(r).wait_recv()

        @pl.when(has_hi)
        def _():
            x_dn(r).wait_recv()

    arrived(0)
    arrived(nr - 1)

    for ok, k in ((y_hi, 0), (y_lo, 1)):
        @pl.when(ok)
        def _(k=k):
            y_edge[k].start()

        @pl.when(jnp.logical_and(ok, has_lo))
        def _(k=k):
            y_far[0][k].start()

        @pl.when(jnp.logical_and(ok, has_hi))
        def _(k=k):
            y_far[1][k].start()

    pass_on(2)
    lane = lax.broadcasted_iota(jnp.int32, (8, LANES), 1)

    def columns(tile):
        at = pl.ds(pl.multiple_of(tile * 8, 8), 8)
        sums = []
        for t in range(nt + 1):
            e = [ext[p, t, at, :] for p in range(10)]
            mid = (e[3] + e[4]) + (e[5] + e[6])
            lo2, hi2 = e[2] + e[1], e[7] + e[8]
            sums.append([mid + (lo2 + e[0]), mid + lo2 + e[7], mid + e[2] + hi2, mid + (hi2 + e[9])])
        for x in range(4):
            h = [sums[t][x] for t in range(nt + 1)]
            after = shifted(nt, roll_all(h, 1), 1, lane)
            before = shifted(nt, roll_all(h, -1), -1, lane)
            for t in range(nt):
                c0[x, t, at, :] = h[t]
                d0[x, t, at, :] = after[t] - before[t]
                s0[x, t, at, :] = after[t] + before[t] - 2.0 * h[t]
        for p in range(6):
            f = [ext[2 + p, t, at, :] for t in range(nt + 1)]
            pair = [a + b for a, b in zip(f, shifted(nt + 1, roll_all(f, 1), 1, lane))]
            quad = [a + b for a, b in zip(pair, shifted(nt + 1, roll_all(pair, 2), 2, lane))]
            back = shifted(nt, roll_all(quad, -3), -3, lane)
            for t in range(nt):
                c2[p, t, at, :] = back[t] + (quad[t] - f[t])

    def curve(tile):
        row = tile * 8
        own = pl.ds(pl.multiple_of(row - 8, 8), 8)
        at = pl.ds(pl.multiple_of(row, 8), 8)
        up, dn = pl.ds(row + 1, 8), pl.ds(row - 1, 8)
        col = []
        for p in range(6):
            parts = []
            for t in range(nt + 1):
                v = [ext[2 + p, t, pl.ds(row + k, 8), :] for k in range(-3, 4)]
                parts.append(((v[0] + v[1]) + (v[2] + v[3])) + ((v[4] + v[5]) + v[6]))
            after = shifted(nt, roll_all(parts, 1), 1, lane)
            before = shifted(nt, roll_all(parts, -1), -1, lane)
            col.append((parts, [a - b for a, b in zip(after, before)], [a + b for a, b in zip(after, before)]))
        best = vmax[...]
        for t in range(nt):
            across = pl.ds(t * LANES, LANES)
            for x in range(4):
                o = ori[x, own, across]
                is0, is1 = o == 0, o == 1

                def pick(a, b, c):
                    return jnp.where(is0, a, jnp.where(is1, b, c))

                h0 = c0[x, t, at, :]
                u0, w0 = c0[x, t, up, :], c0[x, t, dn, :]
                h1 = col[x + 1][0][t]
                u1, w1 = col[x + 2][0][t], col[x][0][t]
                h2 = c2[x + 1, t, at, :]
                u2, w2 = c2[x + 2, t, at, :], c2[x, t, at, :]
                b2u, b2w = c2[x + 1, t, up, :], c2[x + 1, t, dn, :]
                twist2 = (c2[x + 2, t, up, :] - c2[x + 2, t, dn, :]) - (c2[x, t, up, :] - c2[x, t, dn, :])
                centre = pick(h0, h1, h2)
                plus, minus = pick(u0, u1, u2), pick(w0, w1, w2)
                slope_a = 0.5 * (plus - minus)
                bend_a = plus + minus - 2.0 * centre
                slope_b = 0.5 * pick(d0[x, t, at, :], col[x + 1][1][t], b2u - b2w)
                bend_b = pick(s0[x, t, at, :], col[x + 1][2][t] - 2.0 * h1, b2u + b2w - 2.0 * h2)
                twist = pick(d0[x, t, up, :] - d0[x, t, dn, :], col[x + 2][1][t] - col[x][1][t], twist2)
                qa, qb = slope_a * slope_a, slope_b * slope_b
                numer = bend_a * (1.0 + qb) + bend_b * (1.0 + qa) - 0.5 * twist * (slope_a * slope_b)
                inv = lax.rsqrt(1.0 + qa + qb)
                kappa = jnp.where(itf[x, own, across] == 1, numer * (inv * inv * inv), 0.0)
                res[x, own, across] = kappa
                best = jnp.maximum(best, jnp.abs(kappa))
        vmax[...] = best

    for ok, k in ((y_lo, 0), (y_hi, 1)):
        @pl.when(ok)
        def _(k=k):
            y_own[k].wait_recv()
            y_edge[k].wait_recv()

        @pl.when(jnp.logical_and(ok, has_lo))
        def _(k=k):
            y_far[0][k].wait_recv()

        @pl.when(jnp.logical_and(ok, has_hi))
        def _(k=k):
            y_far[1][k].wait_recv()

    pass_on(3)
    load_ori.wait()
    load_itf.wait()

    def edges(i, carry):
        columns(i + jnp.where(i >= 2, nr - 2, 0))
        return carry

    lax.fori_loop(0, 4, edges, 0)
    pass_on(4)

    def middle(tile, carry):
        arrived(tile - 1)
        columns(tile)
        curve(tile - 1)
        return carry

    lax.fori_loop(2, nr, middle, 0)

    def tail(tile, carry):
        curve(tile)
        return carry

    lax.fori_loop(nr - 1, nr + 1, tail, 0)

    r1[me1] = jnp.max(vmax[...], axis=0, keepdims=True)

    def red1(k, sign=1):
        y, at = peer1(steps1[k], sign)
        slot = me1 if sign > 0 else y * ngy + at
        return remote(r1.at[slot], r1.at[slot], r1s.at[k], r1r.at[k], (y * zhi + z_at, at, gz))

    def red2(k, sign=1):
        i = peer2(steps2[k], sign)
        slot = me2 if sign > 0 else i
        return remote(r2.at[slot], r2.at[slot], r2s.at[k], r2r.at[k], (y_at * zhi + i // ngz, gy, lax.rem(i, ngz)))

    for d in range(n1 - 1):
        red1(d).start()
    for d in range(n1 - 1):
        red1(n1 - 2 - d, -1).wait_recv()
    r2[me2] = jnp.max(r1[...], axis=0)
    for d in range(n2 - 1):
        red2(d).start()

    z_own.wait_send()

    def sent_row(r, carry):
        @pl.when(has_hi)
        def _():
            x_up(r).wait_send()

        @pl.when(has_lo)
        def _():
            x_dn(r).wait_send()

        return carry

    lax.fori_loop(0, nr, sent_row, 0)

    @pl.when(has_hi)
    def _():
        z_up[0].wait_send()
        z_up[1].wait_send()

    @pl.when(has_lo)
    def _():
        z_dn[0].wait_send()
        z_dn[1].wait_send()

    for ok, k in ((y_hi, 0), (y_lo, 1)):
        @pl.when(ok)
        def _(k=k):
            y_own[k].wait_send()
            y_edge[k].wait_send()

        @pl.when(jnp.logical_and(ok, has_lo))
        def _(k=k):
            y_far[0][k].wait_send()

        @pl.when(jnp.logical_and(ok, has_hi))
        def _(k=k):
            y_far[1][k].wait_send()

    for d in range(n1 - 1):
        red1(d).wait_send()
    for d in range(n2 - 1):
        red2(n2 - 2 - d, -1).wait_recv()
    peak_ref[...] = jnp.max(r2[...], axis=0)
    for d in range(n2 - 1):
        red2(d).wait_send()


def settle(res, peak, out, peak_out, top, sems):
    copies = [pltpu.make_async_copy(res, out, sems.at[0])]
    for copy in copies:
        copy.start()
    top[0, 0] = jnp.max(peak[...])
    last = pltpu.make_async_copy(top, peak_out, sems.at[1])
    last.start()
    last.wait()
    for copy in copies:
        copy.wait()


def block(sizes, fraction, orientation, interface):
    planes, rows, lanes = fraction.shape
    ngx, ngy, ngz, zhi = sizes
    nt, nr = lanes // LANES, rows // 8
    n1, n2 = (ngx // zhi) * ngy, zhi * ngz
    hops = ngy // 4 + ngx // zhi // 2 + 1
    dma = pltpu.SemaphoreType.DMA
    f32 = jnp.float32
    curvature, peak = pl.pallas_call(
        functools.partial(kernel, sizes),
        out_shape=(
            jax.ShapeDtypeStruct(fraction.shape, f32),
            jax.ShapeDtypeStruct((1, LANES), f32),
        ),
        in_specs=[pl.BlockSpec(memory_space=pl.ANY)] * 3,
        out_specs=(pl.BlockSpec(memory_space=pltpu.VMEM), pl.BlockSpec(memory_space=pltpu.VMEM)),
        scratch_shapes=[
            pltpu.VMEM((10, nt + 1, rows + 16, LANES), f32),
            pltpu.VMEM((4, nt, rows + 16, LANES), f32),
            pltpu.VMEM((4, nt, rows + 16, LANES), f32),
            pltpu.VMEM((4, nt, rows + 16, LANES), f32),
            pltpu.VMEM((6, nt, rows + 16, LANES), f32),
            pltpu.VMEM((planes, rows, lanes), jnp.int32),
            pltpu.VMEM((planes, rows, lanes), jnp.int32),
            pltpu.VMEM((4, 3, 1, LANES), f32),
            pltpu.VMEM((10, 3, 1, LANES), f32),
            pltpu.VMEM((10, 8, LANES), f32),
            pltpu.VMEM((8, LANES), f32),
            pltpu.VMEM((n1, 1, LANES), f32),
            pltpu.VMEM((n2, 1, LANES), f32),
            dma((nt + 2,)),
            dma((2, nr)), dma((2, nr)),
            dma((2,)), dma((2,)),
            dma((2,)), dma((2,)),
            dma((2, 2)), dma((2, 2)),
            dma((5,)), dma((5,)),
            dma((n1,)), dma((n1,)),
            dma((n2,)), dma((n2,)),
            pltpu.SemaphoreType.REGULAR((hops - 1,)),
        ],
        compiler_params=pltpu.CompilerParams(
            collective_id=0, has_side_effects=True, vmem_limit_bytes=55000000
        ),
    )(fraction, orientation, interface)
    curvature, peak = pl.pallas_call(
        settle,
        out_shape=(
            jax.ShapeDtypeStruct(fraction.shape, f32),
            jax.ShapeDtypeStruct((1, 1), f32),
        ),
        in_specs=[pl.BlockSpec(memory_space=pltpu.VMEM), pl.BlockSpec(memory_space=pltpu.VMEM)],
        out_specs=(pl.BlockSpec(memory_space=pl.ANY),) * 2,
        scratch_shapes=[pltpu.SMEM((1, 1), f32), dma((2,))], compiler_params=pltpu.CompilerParams(vmem_limit_bytes=1048576 * 2),
    )(curvature, peak)
    return curvature, peak.reshape(())


def solution(mesh):
    sizes = (mesh.shape["gx"], mesh.shape["gy"], mesh.shape["gz"], min(Z_HI, mesh.shape["gx"]))
    spec = P("gx", "gy", "gz")
    return jax.shard_map(
        functools.partial(block, sizes), mesh=mesh, in_specs=(spec,) * 3, out_specs=(spec, P()), check_vma=False
    )
```
